32 devices in a mesh: dp: 4 (over y, z), ep: 8 (over x, core).
Axes of the slice: x: 4, y: 2, z: 2, core: 2. Of those that a mesh axis runs over, the one named last changes fastest.
The devices are a block of a 4x4x8 slice.
Arguments:
- hidden: bfloat16 [32768, 2048], P(('dp', 'ep')), parts along dimension 0
- w_router: bfloat16 [2048, 64], replicated
- w_gate: bfloat16 [64, 2048, 1408], P('ep')
- w_up: bfloat16 [64, 2048, 1408], P('ep')
- w_down: bfloat16 [64, 1408, 2048], P('ep')
- shared_gate: bfloat16 [2048, 2816], replicated
- shared_up: bfloat16 [2048, 2816], replicated
- shared_down: bfloat16 [2816, 2048], replicated
- top_idx: int32 [32768, 6], P(('dp', 'ep')), parts along dimension 0
- keep_mask: int32 [32768, 6], P(('dp', 'ep')), parts along dimension 0
Outputs:
- output: bfloat16 [32768, 2048], P(('dp', 'ep')), parts along dimension 0
There are 4 independent parts. The reference program is written for one: setup_inputs(seed, part) draws one part's arguments, and reference() takes and returns one part's arrays. A program takes and returns all parts, laid end to end along the dimension named above; an argument that names none is the same for every part.
All inputs are finite; a program needn't handle non-finite values.
Results may differ from the reference program's by a relative error of at most 0.00691113.
Values are sent between devices in bfloat16 or wider.
A program may use at most 768 MiB of HBM per device.

```python
import math
import jax
import jax.numpy as jnp
from jax import lax

HIDDEN = 2048
EXPERTS = 64
EXPERT_FF = 1408
SHARED_FF = 2816
TOP_K = 6
DEV_LIMIT = 6
TOKENS = 1024
GROUP_SIZE = 8
CAPACITY = 192

ROUTE_SCALE = 16.0
PER_DEVICE = EXPERTS // GROUP_SIZE
PART_TOKENS = GROUP_SIZE * TOKENS
ROUTED_GAIN = EXPERTS / (ROUTE_SCALE * math.sqrt(TOP_K))


def draw_routing(route_key):
    k_noise, k_dev, k_exp, k_hot = jax.random.split(route_key, 4)
    expert_ids = jnp.arange(EXPERTS, dtype=jnp.int32)
    noise_int = jax.random.randint(k_noise, (PART_TOKENS, EXPERTS), 0, 256, dtype=jnp.int32)
    dev_bias = jax.random.randint(k_dev, (GROUP_SIZE,), 0, 128, dtype=jnp.int32)
    exp_bias = jax.random.randint(k_exp, (EXPERTS,), 0, 64, dtype=jnp.int32)
    hot_expert = jax.random.randint(k_hot, (), 0, EXPERTS, dtype=jnp.int32)
    bias_all = exp_bias + jnp.repeat(dev_bias, PER_DEVICE) + jnp.where(expert_ids == hot_expert, 1024, 0)
    pair_score = (noise_int + bias_all[None, :]) * EXPERTS + expert_ids[None, :]
    dev_score = jnp.max(pair_score.reshape(PART_TOKENS, GROUP_SIZE, PER_DEVICE), axis=2)
    top_dev = lax.top_k(dev_score, DEV_LIMIT)[1]
    chosen = jnp.any(top_dev[:, :, None] == jnp.arange(GROUP_SIZE, dtype=jnp.int32)[None, None, :], axis=1)
    masked = jnp.where(jnp.repeat(chosen, PER_DEVICE, axis=1), pair_score, -1)
    top_idx = lax.top_k(masked, TOP_K)[1].astype(jnp.int32)

    def rank_pairs(src_pairs):
        onehot = (src_pairs[:, None] == expert_ids[None, :]).astype(jnp.int32)
        return jnp.sum((jnp.cumsum(onehot, axis=0) - 1) * onehot, axis=1)

    pair_rank = lax.map(rank_pairs, top_idx.reshape(GROUP_SIZE, TOKENS * TOP_K))
    keep_mask = (pair_rank < CAPACITY).astype(jnp.int32).reshape(PART_TOKENS, TOP_K)
    return top_idx, keep_mask


def draw_bank(bank_key, mat_shape, std_scale):
    key_list = jax.random.split(bank_key, EXPERTS)
    return lax.map(lambda one_key: (jax.random.normal(one_key, mat_shape, jnp.float32) * std_scale).astype(jnp.bfloat16), key_list)


def draw_matrix(mat_key, mat_shape, std_scale):
    return (jax.random.normal(mat_key, mat_shape, jnp.float32) * std_scale).astype(jnp.bfloat16)


def setup_inputs(seed: int = 0, part: int = 0) -> dict:
    root_key = jax.random.key(seed)
    part_key = jax.random.fold_in(root_key, part)
    k_hidden, k_route = jax.random.split(part_key, 2)
    k_router, k_gate, k_up, k_down, k_sgate, k_sup, k_sdown = jax.random.split(root_key, 7)
    top_idx, keep_mask = draw_routing(k_route)
    in_scale = HIDDEN ** -0.5
    return {
        "hidden": draw_matrix(k_hidden, (PART_TOKENS, HIDDEN), 1.0),
        "w_router": draw_matrix(k_router, (HIDDEN, EXPERTS), 0.5 * in_scale),
        "w_gate": draw_bank(k_gate, (HIDDEN, EXPERT_FF), in_scale),
        "w_up": draw_bank(k_up, (HIDDEN, EXPERT_FF), in_scale),
        "w_down": draw_bank(k_down, (EXPERT_FF, HIDDEN), ROUTED_GAIN * EXPERT_FF ** -0.5),
        "shared_gate": draw_matrix(k_sgate, (HIDDEN, SHARED_FF), in_scale),
        "shared_up": draw_matrix(k_sup, (HIDDEN, SHARED_FF), in_scale),
        "shared_down": draw_matrix(k_sdown, (SHARED_FF, HIDDEN), SHARED_FF ** -0.5),
        "top_idx": top_idx,
        "keep_mask": keep_mask,
    }


def swiglu(tok_rows, gate_w, up_w, down_w):
    h_gate = jnp.dot(tok_rows, gate_w, preferred_element_type=jnp.float32)
    h_up = jnp.dot(tok_rows, up_w, preferred_element_type=jnp.float32)
    act_rows = (jax.nn.silu(h_gate) * h_up).astype(jnp.bfloat16)
    return jnp.dot(act_rows, down_w, preferred_element_type=jnp.float32)


def reference(hidden, w_router, w_gate, w_up, w_down, shared_gate, shared_up, shared_down, top_idx, keep_mask):
    logits = jnp.dot(hidden, w_router, preferred_element_type=jnp.float32)
    router_prob = jax.nn.softmax(logits, axis=-1)
    gate_vals = ROUTE_SCALE * jnp.take_along_axis(router_prob, top_idx, axis=1) * keep_mask.astype(jnp.float32)
    pair_expert = top_idx.reshape(-1)
    pair_kept = keep_mask.reshape(-1) > 0
    pair_gate = gate_vals.reshape(-1)
    pair_token = jnp.arange(PART_TOKENS * TOP_K, dtype=jnp.int32) // TOP_K
    max_rows = GROUP_SIZE * CAPACITY

    def expert_step(routed_acc, per_expert):
        gate_w, up_w, down_w, expert_id = per_expert
        member = pair_kept & (pair_expert == expert_id)
        pair_slot = jnp.where(member, jnp.cumsum(member.astype(jnp.int32)) - 1, max_rows)
        row_token = jnp.zeros((max_rows,), jnp.int32).at[pair_slot].set(pair_token, mode="drop")
        row_gate = jnp.zeros((max_rows,), jnp.float32).at[pair_slot].set(pair_gate, mode="drop")
        expert_out = swiglu(hidden[row_token], gate_w, up_w, down_w).astype(jnp.bfloat16)
        routed_acc = routed_acc.at[row_token].add(row_gate[:, None] * expert_out.astype(jnp.float32))
        return routed_acc, None

    routed = lax.scan(expert_step, jnp.zeros((PART_TOKENS, HIDDEN), jnp.float32), (w_gate, w_up, w_down, jnp.arange(EXPERTS, dtype=jnp.int32)))[0]
    shared = lax.map(lambda tok_block: swiglu(tok_block, shared_gate, shared_up, shared_down), hidden.reshape(GROUP_SIZE, TOKENS, HIDDEN)).reshape(PART_TOKENS, HIDDEN)
    return (shared + routed).astype(jnp.bfloat16)
```

```python
import jax
import jax.numpy as jnp
from jax import lax
from jax.experimental import pallas as pl
from jax.experimental.pallas import tpu as pltpu
from jax.sharding import PartitionSpec as P


ROUTE_SCALE = 16.0
LANES = 128


def route_tables(hidden, w_router, top_idx, keep_mask):
    tokens, top_k = top_idx.shape
    experts = w_router.shape[1]
    width, unroll = 256, 4

    def kernel(x_ref, w_ref, idx_ref, keep_ref, tok_ref, gate_ref, slot_t, parts_t):
        logits = jnp.dot(x_ref[...], w_ref[...], preferred_element_type=jnp.float32)
        top = jnp.max(logits, axis=-1, keepdims=True)
        ex = jnp.exp(logits - top)
        prob = ex / jnp.sum(ex, axis=-1, keepdims=True)
        lane = lax.broadcasted_iota(jnp.int32, (tokens, experts), 1)
        member = jnp.zeros((tokens, experts), jnp.float32)
        for k in range(top_k):
            hit = (idx_ref[:, k:k + 1] == lane) & (keep_ref[:, k:k + 1] > 0)
            member = jnp.where(hit, 1.0, member)
        gates = ROUTE_SCALE * prob * member
        before = lax.broadcasted_iota(jnp.int32, (tokens, tokens), 0) >= lax.broadcasted_iota(jnp.int32, (tokens, tokens), 1)
        rank = jnp.dot(jnp.where(before, 1.0, 0.0).astype(jnp.bfloat16), member.astype(jnp.bfloat16), preferred_element_type=jnp.float32)
        slot = jnp.where(member > 0.0, rank - 1.0, -1.0)
        pad = jnp.zeros((tokens, LANES - experts), jnp.float32)
        slot_t[...] = jnp.transpose(jnp.concatenate([slot, pad], axis=1))[:experts]
        gt = jnp.transpose(jnp.concatenate([gates, pad], axis=1))[:experts]
        g1 = gt.astype(jnp.bfloat16).astype(jnp.float32)
        g2 = (gt - g1).astype(jnp.bfloat16).astype(jnp.float32)
        g3 = (gt - g1 - g2).astype(jnp.bfloat16).astype(jnp.float32)
        parts_t[0] = g1
        parts_t[1] = g2
        parts_t[2] = g3
        col = lax.broadcasted_iota(jnp.int32, (8, tokens), 1)
        row = lax.broadcasted_iota(jnp.int32, (8, tokens), 0)
        base = jnp.where(row == 0, (col // 32).astype(jnp.float32), jnp.where(row == 1, (col % 32).astype(jnp.float32), jnp.where(row == 2, 1.0, 0.0)))
        want = lax.broadcasted_iota(jnp.int32, (width, tokens), 0).astype(jnp.float32)

        @pl.loop(0, experts // unroll)
        def _(i):
            for u in range(unroll):
                e = i * unroll + u
                onehot = jnp.where(slot_t[pl.ds(e, 1), :] == want, 1.0, 0.0).astype(jnp.bfloat16)
                vrows = base
                for q in range(3):
                    vrows = jnp.where(row == 3 + q, parts_t[q, pl.ds(e, 1), :], vrows)
                res = lax.dot_general(vrows.astype(jnp.bfloat16), onehot, (((1,), (1,)), ((), ())), preferred_element_type=jnp.float32)
                tok = jnp.where(res[2:3] > 0.5, res[0:1] * 32.0 + res[1:2], float(tokens))
                tok_ref[pl.ds(e, 1), :] = tok
                gate_ref[pl.ds(e, 1), :] = (res[5:6] + res[4:5]) + res[3:4]

    vmem = pl.BlockSpec(memory_space=pltpu.VMEM)
    return pl.pallas_call(
        kernel,
        out_shape=[jax.ShapeDtypeStruct((experts, width), jnp.float32)] * 2,
        in_specs=[vmem] * 4,
        out_specs=[vmem] * 2,
        scratch_shapes=[
            pltpu.VMEM((experts, tokens), jnp.float32),
            pltpu.VMEM((3, experts, tokens), jnp.float32),
        ],
        compiler_params=pltpu.CompilerParams(vmem_limit_bytes=48 * 1024 * 1024),
        cost_estimate=pl.CostEstimate(flops=20_000_000_000, bytes_accessed=8_000_000, transcendentals=100_000),
    )(hidden, w_router, top_idx, keep_mask)


def split(n, parts):
    return [(n * i // parts, n * (i + 1) // parts) for i in range(parts)]


def expert_pass(ids, xa, xb, tok, gate, w1, w3, w2, cap, b_dtype, G=4):
    T, C, L = xa.shape
    E, D, F = w1.shape
    M = 2 * cap
    S = M + 1
    nU, nD = F // 128, D // 256
    base = (2 * T + 2) * C
    narrow = b_dtype == jnp.bfloat16

    def kernel(ids_ref, tok_ref, gate_ref, xa_ref, xb_ref, w1_ref, w3_ref, w2_ref, oa_ref, ob_ref,
               xv, mem, w1v, w3v, w2v, g, av, xsem, wsem, osem):
        first = [ids_ref[0] * E, ids_ref[1] * E]
        x_refs = (xa_ref, xb_ref)

        def weights(e, p):
            return [pltpu.make_async_copy(src.at[e], dst.at[p], wsem.at[p, i]) for i, (src, dst) in enumerate(((w1_ref, w1v), (w3_ref, w3v), (w2_ref, w2v)))]

        def spread(e, b, c):
            t = tok_ref[first[b] + e, c] + b * (T + 1)
            mem[pl.ds(base + b * cap + c, C, stride=S), :] = xv[t].astype(jnp.float32)

        def convert(j):
            g[j] = mem[base + j * S:base + j * S + M, :].astype(jnp.bfloat16)

        def scatter(e, b, cols):
            vals = []
            for c in cols:
                t = tok_ref[first[b] + e, c] + b * (T + 1)
                at = pl.ds(pl.multiple_of(t * C, C), C)
                vals.append((at, mem[at, :] + gate_ref[first[b] + e, c] * mem[pl.ds(base + b * cap + c, C, stride=S), :]))
            for at, v in vals:
                mem[at, :] = v

        loads = [pltpu.make_async_copy(x_refs[b], xv.at[pl.ds(b * (T + 1), T)], xsem.at[b]) for b in range(2)]
        for c in loads: c.start()
        for c in weights(0, 0): c.start(priority=1)
        for b in range(2):
            xv[b * (T + 1) + T] = jnp.zeros((C, L), xv.dtype)

        @pl.loop(0, (2 * T + 2) // 10)
        def _(i):
            mem[pl.ds(pl.multiple_of(i * 10 * C, 8), 10 * C), :] = jnp.zeros((10 * C, L), jnp.float32)

        for b in range(2):
            loads[b].wait()

            @pl.loop(0, cap // 16)
            def _(i):
                for u in range(16):
                    spread(0, b, i * 16 + u)
        for j in range(C): convert(j)

        @pl.loop(0, C)
        def _(i):
            mem[pl.ds(base + i * S, S), :] = jnp.zeros((S, L), jnp.float32)

        def up_tile(p, n):
            cols = pl.ds(n * L, L)
            rows = jnp.concatenate([g[j] for j in range(C)], axis=1)
            h = jnp.dot(rows, jnp.concatenate([w1v[p, :, cols], w3v[p, :, cols]], axis=1), preferred_element_type=jnp.float32)
            av[n] = (jax.nn.silu(h[:, :L]) * h[:, L:]).astype(jnp.bfloat16)

        def down_tile(p, n):
            act = jnp.concatenate([av[j] for j in range(nU)], axis=1)
            h = jnp.dot(act, w2v[p, :, pl.ds(n * 256, 256)], preferred_element_type=jnp.float32)
            h = h.astype(jnp.bfloat16).astype(jnp.float32)
            for k in range(2):
                mem[pl.ds(base + (2 * n + k) * S, M), :] = h[:, L * k:L * k + L]

        groups = [(b, [q + u for u in range(G)]) for b in range(2) for q in range(0, cap, G)]
        parts = split(len(groups), nU)

        @pl.loop(0, E)
        def _(e):
            p = lax.rem(e, 2)
            prev = jnp.maximum(e - 1, 0)
            ahead = jnp.minimum(e + 1, E - 1)
            for c in weights(e, p): c.wait()

            @pl.when(e + 1 < E)
            def _():
                for c in weights(e + 1, 1 - p): c.start(priority=1)

            for n in range(nU):
                for b, cols in groups[slice(*parts[n])]:
                    scatter(prev, b, cols)
                    for c in cols: spread(ahead, b, c)
                up_tile(p, n)
            for n in range(nD):
                convert(2 * n)
                convert(2 * n + 1)
                down_tile(p, n)

        def out(b):
            if b and narrow:
                return pltpu.make_async_copy(xv.at[pl.ds(0, T)], ob_ref, osem.at[b])
            return pltpu.make_async_copy(mem.at[pl.ds(b * (T + 1) * C, T * C)], (oa_ref, ob_ref)[b], osem.at[b])

        for b in range(2):
            @pl.loop(0, cap // 8)
            def _(i):
                scatter(E - 1, b, [i * 8 + u for u in range(8)])

            if b and narrow:
                @pl.loop(0, T // 8)
                def _(i):
                    for u in range(8):
                        r = i * 8 + u
                        xv[r] = mem[pl.ds(pl.multiple_of((T + 1 + r) * C, C), C), :].astype(b_dtype)
            out(b).start()
        for b in range(2):
            out(b).wait()

    anyspec = pl.BlockSpec(memory_space=pl.ANY)
    smem = pl.BlockSpec(memory_space=pltpu.SMEM)
    rows = E * M
    return pl.pallas_call(
        kernel,
        out_shape=[jax.ShapeDtypeStruct((T * C, L), jnp.float32), jax.ShapeDtypeStruct((T, C, L) if narrow else (T * C, L), b_dtype)],
        in_specs=[smem] * 3 + [anyspec] * 5,
        out_specs=[anyspec] * 2,
        scratch_shapes=[
            pltpu.VMEM((2 * T + 2, C, L), jnp.bfloat16),
            pltpu.VMEM((base + C * S, L), jnp.float32),
            pltpu.VMEM((2, D, F), jnp.bfloat16), pltpu.VMEM((2, D, F), jnp.bfloat16), pltpu.VMEM((2, F, D), jnp.bfloat16),
            pltpu.VMEM((C, M, L), jnp.bfloat16),
            pltpu.VMEM((nU, M, L), jnp.bfloat16),
            pltpu.SemaphoreType.DMA((2,)), pltpu.SemaphoreType.DMA((2, 3)), pltpu.SemaphoreType.DMA((2,)),
        ],
        compiler_params=pltpu.CompilerParams(vmem_limit_bytes=67000000),
        cost_estimate=pl.CostEstimate(flops=rows * D * F * 6, bytes_accessed=E * D * F * 6, transcendentals=rows * F),
    )(ids, tok, gate, xa, xb, w1, w3, w2)


def shared_rows(hidden, gate_w, up_w, down_w, total, piece, rows):
    tokens, width = hidden.shape
    ff = gate_w.shape[1]
    tile = 256
    n_up, n_down = ff // tile, width // tile
    up_parts, down_parts = split(n_up, 4), split(n_down, 2)

    def kernel(x_ref, g_ref, u_ref, d_ref, *rest):
        out_ref, xv, gv, uv, dv, act, yv, sem, usem, dsem, osem = rest[-11:]
        load_x = pltpu.make_async_copy(x_ref.at[pl.ds(piece * rows, rows)], xv, sem)
        load_x.start()

        def up_loads(i):
            cols = pl.ds(up_parts[i][0] * tile, (up_parts[i][1] - up_parts[i][0]) * tile)
            return [pltpu.make_async_copy(src.at[:, cols], dst.at[:, cols], usem.at[i, k]) for k, (src, dst) in enumerate(((g_ref, gv), (u_ref, uv)))]

        def down_loads(i):
            cols = pl.ds(down_parts[i][0] * tile, (down_parts[i][1] - down_parts[i][0]) * tile)
            return pltpu.make_async_copy(d_ref.at[:, cols], dv.at[:, cols], dsem.at[i])

        chunks = [up_loads(i) for i in range(len(up_parts))] + [[down_loads(i)] for i in range(len(down_parts))]

        def begin(i):
            if i < len(chunks):
                for c in chunks[i]:
                    c.start()

        def arrive(i):
            for c in chunks[i]:
                c.wait()
            begin(i + 2)

        begin(0)
        load_x.wait()
        begin(1)
        for i, (lo, hi) in enumerate(up_parts):
            arrive(i)
            for n in range(lo, hi):
                cols = slice(n * tile, (n + 1) * tile)
                h_gate = jnp.dot(xv[...], gv[:, cols], preferred_element_type=jnp.float32)
                h_up = jnp.dot(xv[...], uv[:, cols], preferred_element_type=jnp.float32)
                act[:, cols] = (jax.nn.silu(h_gate) * h_up).astype(jnp.bfloat16)

        def store(i):
            cols = pl.ds(down_parts[i][0] * tile, (down_parts[i][1] - down_parts[i][0]) * tile)
            return pltpu.make_async_copy(yv.at[:, cols], out_ref.at[pl.ds(piece * rows, rows), cols], osem.at[i])

        for i, (lo, hi) in enumerate(down_parts):
            arrive(len(up_parts) + i)
            for n in range(lo, hi):
                cols = slice(n * tile, (n + 1) * tile)
                yv[:, cols] = jnp.dot(act[...], dv[:, cols], preferred_element_type=jnp.float32)
            store(i).start()
        for i in range(len(down_parts)):
            store(i).wait()

    operands = [hidden, gate_w, up_w, down_w] + ([] if total is None else [total])
    anyspec = pl.BlockSpec(memory_space=pl.ANY)
    return pl.pallas_call(
        kernel,
        out_shape=jax.ShapeDtypeStruct((tokens, width), jnp.float32),
        in_specs=[anyspec] * len(operands),
        out_specs=anyspec,
        scratch_shapes=[
            pltpu.VMEM((rows, width), jnp.bfloat16),
            pltpu.VMEM((width, ff), jnp.bfloat16), pltpu.VMEM((width, ff), jnp.bfloat16), pltpu.VMEM((ff, width), jnp.bfloat16),
            pltpu.VMEM((rows, ff), jnp.bfloat16), pltpu.VMEM((rows, width), jnp.float32),
            pltpu.SemaphoreType.DMA, pltpu.SemaphoreType.DMA((len(up_parts), 2)), pltpu.SemaphoreType.DMA((len(down_parts),)), pltpu.SemaphoreType.DMA((len(down_parts),)),
        ],
        input_output_aliases={} if total is None else {4: 0},
        compiler_params=pltpu.CompilerParams(vmem_limit_bytes=67000000),
        cost_estimate=pl.CostEstimate(flops=rows * width * ff * 6, bytes_accessed=width * ff * 6, transcendentals=rows * ff),
    )(*operands)


def finish(shared, pa, q, r1, r2, r3):
    tokens, width = shared.shape
    rows = 128
    C = width // LANES
    S = rows + 8

    def kernel(ys_ref, pa_ref, q_ref, r1_ref, r2_ref, r3_ref, out_ref, buf):
        @pl.loop(0, rows // 8)
        def _(i):
            for u in range(8):
                r = i * 8 + u
                v = pa_ref[r]
                for ref in (q_ref, r1_ref, r2_ref, r3_ref):
                    v = v + ref[r].astype(jnp.float32)
                buf[pl.ds(r, C, stride=S), :] = v

        for j in range(C):
            cols = slice(j * LANES, (j + 1) * LANES)
            out_ref[:, cols] = (ys_ref[:, cols] + buf[j * S:j * S + rows, :]).astype(jnp.bfloat16)

    plain = pl.BlockSpec((rows, width), lambda i: (i, 0))
    tile = pl.BlockSpec((rows, C, LANES), lambda i: (i, 0, 0))
    return pl.pallas_call(
        kernel,
        grid=(tokens // rows,),
        out_shape=jax.ShapeDtypeStruct((tokens, width), jnp.bfloat16),
        in_specs=[plain] + [tile] * 5,
        out_specs=plain,
        scratch_shapes=[pltpu.VMEM((C * S, LANES), jnp.float32)],
        compiler_params=pltpu.CompilerParams(vmem_limit_bytes=67000000),
        cost_estimate=pl.CostEstimate(flops=tokens * width * 6, bytes_accessed=tokens * width * 20, transcendentals=0),
    )(shared, pa, q, r1, r2, r3)


def after(value, *deps):
    return lax.optimization_barrier((value, deps))[0]


def solution(mesh):
    n_dev = mesh.shape["ep"]
    chips = n_dev // 2
    tok_spec = P(("dp", "ep"), None)
    bank_spec = P("ep", None, None)
    near = [(2 * c + k, 2 * ((c + (-1 if k == 0 else 1)) % chips) + k) for c in range(chips) for k in range(2)]
    far = [(d, s) for s, d in near]
    across = [(2 * c + k, 2 * ((c + 2) % chips) + k) for c in range(chips) for k in range(2)]
    swap = [(2 * c + k, 2 * c + 1 - k) for c in range(chips) for k in range(2)]

    def device_fn(hidden, w_router, w_gate, w_up, w_down, shared_gate, shared_up, shared_down, top_idx, keep_mask):
        tokens, top_k = top_idx.shape
        width = hidden.shape[1]
        experts = w_router.shape[1]
        per_dev = w_gate.shape[0]
        cap = 8 * ((top_k * tokens + 4 * experts - 1) // (4 * experts))
        me = lax.axis_index("ep")
        chip, core = me // 2, me % 2

        def perm(v, p):
            return lax.ppermute(v, "ep", p)

        x0 = hidden.reshape(tokens, width // LANES, LANES)
        x1 = perm(x0, near)
        tok, gate = route_tables(after(hidden, x0), w_router, top_idx, keep_mask)
        table = jnp.stack([tok, gate], axis=0).reshape(2, n_dev, per_dev, tok.shape[1])
        table = lax.all_to_all(table, "ep", 1, 1, tiled=False)
        table = table.reshape(2, experts, tok.shape[1])[:, :, :cap]
        tok_all, gate_all = table[0].astype(jnp.int32), table[1]

        pieces = 4
        step = tokens // pieces

        def shared_piece(i, total, dep):
            return shared_rows(after(hidden, dep), shared_gate, shared_up, shared_down, total, i, step)

        x0s = perm(x0, swap)
        x1s = perm(x1, swap)
        x3 = perm(x1, near)
        x2 = perm(after(x0, x1), far)
        x3s = perm(x3, swap)
        x2s = perm(x2, swap)

        dirn = jnp.where(core == 0, 1, -1)

        def src(off, k):
            return 2 * ((chip + off + chips) % chips) + k

        def one_pass(xa, xb, off_a, off_b, b_dtype=jnp.float32):
            ids = jnp.stack([src(off_a, core), src(off_b, 1 - core)]).astype(jnp.int32)
            sums = expert_pass(ids, xa, xb, tok_all, gate_all, w_gate, w_up, w_down, cap, b_dtype)
            return [v.reshape(xa.shape) for v in sums]

        def add(pa, q, dep):
            return (after(pa, dep) + q).astype(jnp.bfloat16)

        y = shared_piece(0, None, tok)
        y = shared_piece(1, y, y)
        pa1, pb1 = one_pass(after(x1, y, x1s), x1s, dirn, -dirn)
        q1 = perm(pb1, swap)
        pa2, pb2 = one_pass(after(x3, pa1), x3s, 2, 2)
        q2 = perm(pb2, swap)
        c1 = add(pa1, q1, pa2)
        r1 = perm(c1, far)
        c2 = add(pa2, q2, c1)
        r2 = perm(c2, across)
        pa3, pb3 = one_pass(after(x2, c2), x2s, -dirn, dirn)
        q3 = perm(pb3, swap)
        y = shared_piece(2, y, pa3)
        c3 = add(pa3, q3, y)
        r3 = perm(c3, near)
        pa4, pb4 = one_pass(after(x0, c3), x0s, 0, 0, jnp.bfloat16)
        q4 = perm(pb4, swap)
        y = shared_piece(3, y, (pa4, pb4))
        return finish(y, pa4, q4, r1, r2, r3)

    return jax.shard_map(device_fn, mesh=mesh, in_specs=(tok_spec, P(), bank_spec, bank_spec, bank_spec, P(), P(), P(), tok_spec, tok_spec), out_specs=tok_spec, check_vma=False)
```

```python
import jax
import jax.numpy as jnp
from jax import lax
from jax.experimental import pallas as pl
from jax.experimental.pallas import tpu as pltpu
from jax.sharding import PartitionSpec as P


ROUTE_SCALE = 16.0
LANES = 128


def route_tables(hidden, w_router, top_idx, keep_mask):
    tokens, top_k = top_idx.shape
    experts = w_router.shape[1]
    width, unroll = 256, 4

    def kernel(x_ref, w_ref, idx_ref, keep_ref, tok_ref, gate_ref, slot_t, parts_t):
        logits = jnp.dot(x_ref[...], w_ref[...], preferred_element_type=jnp.float32)
        top = jnp.max(logits, axis=-1, keepdims=True)
        ex = jnp.exp(logits - top)
        prob = ex / jnp.sum(ex, axis=-1, keepdims=True)
        lane = lax.broadcasted_iota(jnp.int32, (tokens, experts), 1)
        member = jnp.zeros((tokens, experts), jnp.float32)
        for k in range(top_k):
            hit = (idx_ref[:, k:k + 1] == lane) & (keep_ref[:, k:k + 1] > 0)
            member = jnp.where(hit, 1.0, member)
        gates = ROUTE_SCALE * prob * member
        before = lax.broadcasted_iota(jnp.int32, (tokens, tokens), 0) >= lax.broadcasted_iota(jnp.int32, (tokens, tokens), 1)
        rank = jnp.dot(jnp.where(before, 1.0, 0.0).astype(jnp.bfloat16), member.astype(jnp.bfloat16), preferred_element_type=jnp.float32)
        slot = jnp.where(member > 0.0, rank - 1.0, -1.0)
        pad = jnp.zeros((tokens, LANES - experts), jnp.float32)
        slot_t[...] = jnp.transpose(jnp.concatenate([slot, pad], axis=1))[:experts]
        gt = jnp.transpose(jnp.concatenate([gates, pad], axis=1))[:experts]
        g1 = gt.astype(jnp.bfloat16).astype(jnp.float32)
        g2 = (gt - g1).astype(jnp.bfloat16).astype(jnp.float32)
        g3 = (gt - g1 - g2).astype(jnp.bfloat16).astype(jnp.float32)
        parts_t[0] = g1
        parts_t[1] = g2
        parts_t[2] = g3
        col = lax.broadcasted_iota(jnp.int32, (8, tokens), 1)
        row = lax.broadcasted_iota(jnp.int32, (8, tokens), 0)
        base = jnp.where(row == 0, (col // 32).astype(jnp.float32), jnp.where(row == 1, (col % 32).astype(jnp.float32), jnp.where(row == 2, 1.0, 0.0)))
        want = lax.broadcasted_iota(jnp.int32, (width, tokens), 0).astype(jnp.float32)

        @pl.loop(0, experts // unroll)
        def _(i):
            for u in range(unroll):
                e = i * unroll + u
                onehot = jnp.where(slot_t[pl.ds(e, 1), :] == want, 1.0, 0.0).astype(jnp.bfloat16)
                vrows = base
                for q in range(3):
                    vrows = jnp.where(row == 3 + q, parts_t[q, pl.ds(e, 1), :], vrows)
                res = lax.dot_general(vrows.astype(jnp.bfloat16), onehot, (((1,), (1,)), ((), ())), preferred_element_type=jnp.float32)
                tok = jnp.where(res[2:3] > 0.5, res[0:1] * 32.0 + res[1:2], float(tokens))
                tok_ref[pl.ds(e, 1), :] = tok
                gate_ref[pl.ds(e, 1), :] = (res[5:6] + res[4:5]) + res[3:4]

    vmem = pl.BlockSpec(memory_space=pltpu.VMEM)
    return pl.pallas_call(
        kernel,
        out_shape=[jax.ShapeDtypeStruct((experts, width), jnp.float32)] * 2,
        in_specs=[vmem] * 4,
        out_specs=[vmem] * 2,
        scratch_shapes=[
            pltpu.VMEM((experts, tokens), jnp.float32),
            pltpu.VMEM((3, experts, tokens), jnp.float32),
        ],
        compiler_params=pltpu.CompilerParams(vmem_limit_bytes=48 * 1024 * 1024),
        cost_estimate=pl.CostEstimate(flops=20_000_000_000, bytes_accessed=8_000_000, transcendentals=100_000),
    )(hidden, w_router, top_idx, keep_mask)


def split(n, parts):
    return [(n * i // parts, n * (i + 1) // parts) for i in range(parts)]


def expert_pass(ids, xa, xb, tok, gate, w1, w3, w2, cap, b_dtype, G=4):
    T, C, L = xa.shape
    E, D, F = w1.shape
    M = 2 * cap
    S = M + 1
    nU, nD = F // 128, D // 256
    base = (2 * T + 2) * C
    mark = -(-(base + C * S) // 8) * 8
    narrow = b_dtype == jnp.bfloat16

    def kernel(ids_ref, tok_all, gate_all, xa_ref, xb_ref, w1_ref, w3_ref, w2_ref, oa_ref, ob_ref,
               xv, mem, w1v, w3v, w2v, g, av, tok_ref, gate_ref, xsem, wsem, osem, tsem):
        first = [0, E]
        lists = [pltpu.make_async_copy(src.at[pl.ds(pl.multiple_of(ids_ref[b] * E, E), E)], dst.at[pl.ds(b * E, E)], tsem.at[b, i]) for b in range(2) for i, (src, dst) in enumerate(((tok_all, tok_ref), (gate_all, gate_ref)))]
        for c in lists: c.start()
        x_refs = (xa_ref, xb_ref)

        def weights(e, p):
            return [pltpu.make_async_copy(src.at[e], dst.at[p], wsem.at[p, i]) for i, (src, dst) in enumerate(((w1_ref, w1v), (w3_ref, w3v), (w2_ref, w2v)))]

        def spread(e, b, c):
            t = tok_ref[first[b] + e, c] + b * (T + 1)
            mem[pl.ds(base + b * cap + c, C, stride=S), :] = xv[t].astype(jnp.float32)

        def convert(j):
            g[j] = mem[base + j * S:base + j * S + M, :].astype(jnp.bfloat16)

        def scatter(e, b, cols):
            vals = []
            for c in cols:
                t = tok_ref[first[b] + e, c] + b * (T + 1)
                at = pl.ds(pl.multiple_of(t * C, C), C)
                vals.append((at, mem[at, :] + gate_ref[first[b] + e, c] * mem[pl.ds(base + b * cap + c, C, stride=S), :]))
            for at, v in vals:
                mem[at, :] = v

        loads = [pltpu.make_async_copy(x_refs[b], xv.at[pl.ds(b * (T + 1), T)], xsem.at[b]) for b in range(2)]
        for c in loads: c.start()
        for c in weights(0, 0): c.start(priority=1)
        for b in range(2):
            xv[b * (T + 1) + T] = jnp.zeros((C, L), xv.dtype)

        @pl.loop(0, (2 * T + 2) // 10)
        def _(i):
            mem[pl.ds(pl.multiple_of(i * 10 * C, 8), 10 * C), :] = jnp.zeros((10 * C, L), jnp.float32)

        for c in lists: c.wait()
        for b in range(2):
            loads[b].wait()

            @pl.loop(0, cap // 16)
            def _(i):
                for u in range(16):
                    spread(0, b, i * 16 + u)
        for j in range(C): convert(j)

        @pl.loop(0, C)
        def _(i):
            mem[pl.ds(base + i * S, S), :] = jnp.zeros((S, L), jnp.float32)

        def up_tile(p, n, lo, hi):
            cols = pl.ds(n * L, L)
            rows = jnp.concatenate([g[j, lo:hi] for j in range(C)], axis=1)
            h = jnp.dot(rows, jnp.concatenate([w1v[p, :, cols], w3v[p, :, cols]], axis=1), preferred_element_type=jnp.float32)
            av[n, lo:hi] = (jax.nn.silu(h[:, :L]) * h[:, L:]).astype(jnp.bfloat16)
            mem[pl.ds(mark, 8), :] = h[:8, :L]

        def down_tile(p, n):
            act = jnp.concatenate([av[j] for j in range(nU)], axis=1)
            h = jnp.dot(act, w2v[p, :, pl.ds(n * 256, 256)], preferred_element_type=jnp.float32)
            h = h.astype(jnp.bfloat16).astype(jnp.float32)
            for k in range(2):
                mem[pl.ds(base + (2 * n + k) * S, M), :] = h[:, L * k:L * k + L]

        groups = [(b, [q + u for u in range(G)]) for b in range(2) for q in range(0, cap, G)]
        parts = split(len(groups), nU)

        @pl.loop(0, E)
        def _(e):
            p = lax.rem(e, 2)
            prev = jnp.maximum(e - 1, 0)
            ahead = jnp.minimum(e + 1, E - 1)
            for c in weights(e, p): c.wait()

            @pl.when(e + 1 < E)
            def _():
                for c in weights(e + 1, 1 - p): c.start(priority=1)

            for n in range(nU):
                for b, cols in groups[slice(*parts[n])]:
                    scatter(prev, b, cols)
                    for c in cols: spread(ahead, b, c)
                if n > 0:
                    up_tile(p, n, 0, M)
                else:
                    up_tile(p, n, 0, M // 2)
                    up_tile(p, n, M // 2, M)
            for n in range(nD):
                convert(2 * n)
                convert(2 * n + 1)
                down_tile(p, n)

        def out(b):
            if b and narrow:
                return pltpu.make_async_copy(xv.at[pl.ds(0, T)], ob_ref, osem.at[b])
            return pltpu.make_async_copy(mem.at[pl.ds(b * (T + 1) * C, T * C)], (oa_ref, ob_ref)[b], osem.at[b])

        for b in range(2):
            @pl.loop(0, cap // 8)
            def _(i):
                scatter(E - 1, b, [i * 8 + u for u in range(8)])

            if b and narrow:
                @pl.loop(0, T // 8)
                def _(i):
                    for u in range(8):
                        r = i * 8 + u
                        xv[r] = mem[pl.ds(pl.multiple_of((T + 1 + r) * C, C), C), :].astype(b_dtype)
            out(b).start()
        for b in range(2):
            out(b).wait()

    anyspec = pl.BlockSpec(memory_space=pl.ANY)
    smem = pl.BlockSpec(memory_space=pltpu.SMEM)
    rows = E * M
    return pl.pallas_call(
        kernel,
        out_shape=[jax.ShapeDtypeStruct((T * C, L), jnp.float32), jax.ShapeDtypeStruct((T, C, L) if narrow else (T * C, L), b_dtype)],
        in_specs=[smem] + [anyspec] * 7,
        out_specs=[anyspec] * 2,
        scratch_shapes=[
            pltpu.VMEM((2 * T + 2, C, L), jnp.bfloat16),
            pltpu.VMEM((mark + 8, L), jnp.float32),
            pltpu.VMEM((2, D, F), jnp.bfloat16), pltpu.VMEM((2, D, F), jnp.bfloat16), pltpu.VMEM((2, F, D), jnp.bfloat16),
            pltpu.VMEM((C, M, L), jnp.bfloat16),
            pltpu.VMEM((nU, M, L), jnp.bfloat16),
            pltpu.SMEM((2 * E, tok.shape[1]), jnp.int32), pltpu.SMEM((2 * E, tok.shape[1]), jnp.float32),
            pltpu.SemaphoreType.DMA((2,)), pltpu.SemaphoreType.DMA((2, 3)), pltpu.SemaphoreType.DMA((2,)), pltpu.SemaphoreType.DMA((2, 2)),
        ],
        compiler_params=pltpu.CompilerParams(vmem_limit_bytes=67000000),
        cost_estimate=pl.CostEstimate(flops=rows * D * F * 6, bytes_accessed=E * D * F * 6, transcendentals=rows * F),
    )(ids, tok, gate, xa, xb, w1, w3, w2)


def shared_rows(hidden, gate_w, up_w, down_w, total, row0, rows):
    tokens, width = hidden.shape
    ff = gate_w.shape[1]
    tile = 256
    n_up, n_down = ff // tile, width // tile
    up_parts, down_parts = split(n_up, 4), split(n_down, 2)

    def kernel(x_ref, g_ref, u_ref, d_ref, *rest):
        out_ref, xv, gv, uv, dv, act, yv, sem, usem, dsem, osem = rest[-11:]
        load_x = pltpu.make_async_copy(x_ref.at[pl.ds(row0, rows)], xv, sem)
        load_x.start()

        def up_loads(i):
            cols = pl.ds(up_parts[i][0] * tile, (up_parts[i][1] - up_parts[i][0]) * tile)
            return [pltpu.make_async_copy(src.at[:, cols], dst.at[:, cols], usem.at[i, k]) for k, (src, dst) in enumerate(((g_ref, gv), (u_ref, uv)))]

        def down_loads(i):
            cols = pl.ds(down_parts[i][0] * tile, (down_parts[i][1] - down_parts[i][0]) * tile)
            return pltpu.make_async_copy(d_ref.at[:, cols], dv.at[:, cols], dsem.at[i])

        chunks = [up_loads(i) for i in range(len(up_parts))] + [[down_loads(i)] for i in range(len(down_parts))]

        def begin(i):
            if i < len(chunks):
                for c in chunks[i]:
                    c.start()

        def arrive(i):
            for c in chunks[i]:
                c.wait()
            begin(i + 2)

        begin(0)
        load_x.wait()
        begin(1)
        for i, (lo, hi) in enumerate(up_parts):
            arrive(i)
            for n in range(lo, hi):
                cols = slice(n * tile, (n + 1) * tile)
                h_gate = jnp.dot(xv[...], gv[:, cols], preferred_element_type=jnp.float32)
                h_up = jnp.dot(xv[...], uv[:, cols], preferred_element_type=jnp.float32)
                act[:, cols] = (jax.nn.silu(h_gate) * h_up).astype(jnp.bfloat16)

        def store(i):
            cols = pl.ds(down_parts[i][0] * tile, (down_parts[i][1] - down_parts[i][0]) * tile)
            return pltpu.make_async_copy(yv.at[:, cols], out_ref.at[pl.ds(row0, rows), cols], osem.at[i])

        for i, (lo, hi) in enumerate(down_parts):
            arrive(len(up_parts) + i)
            for n in range(lo, hi):
                cols = slice(n * tile, (n + 1) * tile)
                yv[:, cols] = jnp.dot(act[...], dv[:, cols], preferred_element_type=jnp.float32)
            store(i).start()
        for i in range(len(down_parts)):
            store(i).wait()

    operands = [hidden, gate_w, up_w, down_w] + ([] if total is None else [total])
    anyspec = pl.BlockSpec(memory_space=pl.ANY)
    return pl.pallas_call(
        kernel,
        out_shape=jax.ShapeDtypeStruct((tokens, width), jnp.float32),
        in_specs=[anyspec] * len(operands),
        out_specs=anyspec,
        scratch_shapes=[
            pltpu.VMEM((rows, width), jnp.bfloat16),
            pltpu.VMEM((width, ff), jnp.bfloat16), pltpu.VMEM((width, ff), jnp.bfloat16), pltpu.VMEM((ff, width), jnp.bfloat16),
            pltpu.VMEM((rows, ff), jnp.bfloat16), pltpu.VMEM((rows, width), jnp.float32),
            pltpu.SemaphoreType.DMA, pltpu.SemaphoreType.DMA((len(up_parts), 2)), pltpu.SemaphoreType.DMA((len(down_parts),)), pltpu.SemaphoreType.DMA((len(down_parts),)),
        ],
        input_output_aliases={} if total is None else {4: 0},
        compiler_params=pltpu.CompilerParams(vmem_limit_bytes=67000000),
        cost_estimate=pl.CostEstimate(flops=rows * width * ff * 6, bytes_accessed=width * ff * 6, transcendentals=rows * ff),
    )(*operands)


def finish(shared, pa, q, r1, r2, r3):
    tokens, width = shared.shape
    n, depth = 16, 6
    rows = tokens // n
    C = width // LANES
    S = rows + 1

    def kernel(ys_ref, pa_ref, q_ref, r1_ref, r2_ref, r3_ref, out_ref, yv, pv, rv, ov, buf, lsem, osem):
        def loads(i):
            part = pl.ds(i * rows, rows)
            copies = [(ys_ref.at[part], yv.at[part]), (pa_ref.at[part], pv.at[part])]
            copies += [(src.at[part], rv.at[k, part]) for k, src in enumerate((q_ref, r1_ref, r2_ref, r3_ref))]
            return [pltpu.make_async_copy(src, dst, lsem.at[i, k]) for k, (src, dst) in enumerate(copies)]

        def store(i):
            part = pl.ds(i * rows, rows)
            return pltpu.make_async_copy(ov.at[part], out_ref.at[part], osem.at[i])

        for i in range(depth):
            for c in loads(i): c.start()
        for i in range(n):
            for c in loads(i): c.wait()
            if i + depth < n:
                for c in loads(i + depth): c.start()

            @pl.loop(0, rows // 8)
            def _(k):
                for u in range(8):
                    r = i * rows + k * 8 + u
                    v = pv[r]
                    for t in range(4):
                        v = v + rv[t, r].astype(jnp.float32)
                    buf[pl.ds(k * 8 + u, C, stride=S), :] = v

            for j in range(C):
                at, cols = slice(i * rows, (i + 1) * rows), slice(j * LANES, (j + 1) * LANES)
                ov[at, cols] = (yv[at, cols] + buf[j * S:j * S + rows, :]).astype(jnp.bfloat16)
            store(i).start()
        for i in range(n):
            store(i).wait()

    anyspec = pl.BlockSpec(memory_space=pl.ANY)
    return pl.pallas_call(
        kernel,
        out_shape=jax.ShapeDtypeStruct((tokens, width), jnp.bfloat16),
        in_specs=[anyspec] * 6,
        out_specs=anyspec,
        scratch_shapes=[
            pltpu.VMEM((tokens, width), jnp.float32), pltpu.VMEM(pa.shape, jnp.float32), pltpu.VMEM((4,) + q.shape, jnp.bfloat16),
            pltpu.VMEM((tokens, width), jnp.bfloat16), pltpu.VMEM((C * S, LANES), jnp.float32),
            pltpu.SemaphoreType.DMA((n, 6)), pltpu.SemaphoreType.DMA((n,)),
        ],
        compiler_params=pltpu.CompilerParams(vmem_limit_bytes=67000000),
        cost_estimate=pl.CostEstimate(flops=tokens * width * 6, bytes_accessed=tokens * width * 20, transcendentals=0),
    )(shared, pa, q, r1, r2, r3)


def add_partials(pa, q):
    tokens, C, L = pa.shape
    n, depth = 16, 6
    rows = tokens // n

    def kernel(a_ref, q_ref, out_ref, av, qv, cv, asem, qsem, csem):
        part = [pl.ds(i * rows, rows) for i in range(n)]

        def loads(i):
            return [pltpu.make_async_copy(a_ref.at[part[i]], av.at[part[i]], asem.at[i]), pltpu.make_async_copy(q_ref.at[part[i]], qv.at[part[i]], qsem.at[i])]

        def store(i):
            return pltpu.make_async_copy(cv.at[part[i]], out_ref.at[part[i]], csem.at[i])

        for i in range(depth):
            for c in loads(i): c.start()
        for i in range(n):
            for c in loads(i): c.wait()
            if i + depth < n:
                for c in loads(i + depth): c.start()

            @pl.loop(0, rows // 8)
            def _(k):
                at = pl.ds(i * rows + k * 8, 8)
                cv[at] = (av[at] + qv[at]).astype(jnp.bfloat16)

            store(i).start()
        for i in range(n):
            store(i).wait()

    anyspec = pl.BlockSpec(memory_space=pl.ANY)
    return pl.pallas_call(
        kernel,
        out_shape=jax.ShapeDtypeStruct(pa.shape, jnp.bfloat16),
        in_specs=[anyspec] * 2,
        out_specs=anyspec,
        scratch_shapes=[
            pltpu.VMEM(pa.shape, jnp.float32), pltpu.VMEM(pa.shape, jnp.float32), pltpu.VMEM(pa.shape, jnp.bfloat16),
            pltpu.SemaphoreType.DMA((n,)), pltpu.SemaphoreType.DMA((n,)), pltpu.SemaphoreType.DMA((n,)),
        ],
        compiler_params=pltpu.CompilerParams(vmem_limit_bytes=67000000),
        cost_estimate=pl.CostEstimate(flops=tokens * C * L, bytes_accessed=tokens * C * L * 10, transcendentals=0),
    )(pa, q)


def after(value, *deps):
    return lax.optimization_barrier((value, deps))[0]


def solution(mesh):
    n_dev = mesh.shape["ep"]
    chips = n_dev // 2
    tok_spec = P(("dp", "ep"), None)
    bank_spec = P("ep", None, None)
    near = [(2 * c + k, 2 * ((c + (-1 if k == 0 else 1)) % chips) + k) for c in range(chips) for k in range(2)]
    far = [(d, s) for s, d in near]
    across = [(2 * c + k, 2 * ((c + 2) % chips) + k) for c in range(chips) for k in range(2)]
    swap = [(2 * c + k, 2 * c + 1 - k) for c in range(chips) for k in range(2)]

    def device_fn(hidden, w_router, w_gate, w_up, w_down, shared_gate, shared_up, shared_down, top_idx, keep_mask):
        tokens, top_k = top_idx.shape
        width = hidden.shape[1]
        experts = w_router.shape[1]
        per_dev = w_gate.shape[0]
        cap = 8 * ((top_k * tokens + 4 * experts - 1) // (4 * experts))
        me = lax.axis_index("ep")
        chip, core = me // 2, me % 2

        def perm(v, p):
            return lax.ppermute(v, "ep", p)

        x0 = hidden.reshape(tokens, width // LANES, LANES)
        x1 = perm(x0, near)
        tok, gate = route_tables(after(hidden, x0), w_router, top_idx, keep_mask)
        table = jnp.stack([tok, gate], axis=0).reshape(2, n_dev, per_dev, tok.shape[1])
        table = lax.all_to_all(table, "ep", 1, 1, tiled=False)
        table = table.reshape(2, experts, tok.shape[1])
        tok_all, gate_all = table[0].astype(jnp.int32), table[1]

        def shared_piece(total, dep, lo, hi):
            return shared_rows(after(hidden, dep), shared_gate, shared_up, shared_down, total, lo * tokens // 4, (hi - lo) * tokens // 4)

        x0s = perm(x0, swap)
        x1s = perm(x1, swap)
        x3 = perm(x1, near)
        x3s = perm(x3, swap)

        dirn = jnp.where(core == 0, 1, -1)

        def src(off, k):
            return 2 * ((chip + off + chips) % chips) + k

        def one_pass(xa, xb, off_a, off_b, b_dtype=jnp.float32):
            ids = jnp.stack([src(off_a, core), src(off_b, 1 - core)]).astype(jnp.int32)
            sums = expert_pass(ids, xa, xb, tok_all, gate_all, w_gate, w_up, w_down, cap, b_dtype)
            return [v.reshape(xa.shape) for v in sums]

        def add(pa, q, dep):
            return add_partials(after(pa, dep), q)

        y = shared_piece(None, tok, 0, 2)
        pa1, pb1 = one_pass(after(x1, y, x1s), x1s, dirn, -dirn)
        x2 = perm(after(x0, pa1), far)
        x2s = perm(x2, swap)
        q1 = perm(pb1, swap)
        pa2, pb2 = one_pass(after(x3, pa1), x3s, 2, 2)
        q2 = perm(pb2, swap)
        c1 = add(pa1, q1, pa2)
        r1 = perm(c1, far)
        c2 = add(pa2, q2, c1)
        r2 = perm(c2, across)
        pa3, pb3 = one_pass(after(x2, c2), x2s, -dirn, dirn)
        q3 = perm(pb3, swap)
        y = shared_piece(y, pa3, 2, 3)
        c3 = add(pa3, q3, y)
        r3 = perm(c3, near)
        pa4, pb4 = one_pass(after(x0, c3), x0s, 0, 0, jnp.bfloat16)
        q4 = perm(pb4, swap)
        y = shared_piece(y, (pa4, pb4), 3, 4)
        return finish(y, pa4, q4, r1, r2, r3)

    return jax.shard_map(device_fn, mesh=mesh, in_specs=(tok_spec, P(), bank_spec, bank_spec, bank_spec, P(), P(), P(), tok_spec, tok_spec), out_specs=tok_spec, check_vma=False)
```

```python
import jax
import jax.numpy as jnp
from jax import lax
from jax.experimental import pallas as pl
from jax.experimental.pallas import tpu as pltpu
from jax.sharding import PartitionSpec as P


ROUTE_SCALE = 16.0
LANES = 128
SPARE = 8


def route_tables(hidden, w_router, top_idx, keep_mask, cap):
    tokens, top_k = top_idx.shape
    experts = w_router.shape[1]
    width, unroll = cap, 4

    def kernel(x_ref, w_ref, idx_ref, keep_ref, tok_ref, gate_ref, slot_t, parts_t, xv, sem):
        load = pltpu.make_async_copy(x_ref, xv, sem)
        load.start()
        lane = lax.broadcasted_iota(jnp.int32, (tokens, experts), 1)
        member = jnp.zeros((tokens, experts), jnp.float32)
        for k in range(top_k):
            hit = (idx_ref[:, k:k + 1] == lane) & (keep_ref[:, k:k + 1] > 0)
            member = jnp.where(hit, 1.0, member)
        before = lax.broadcasted_iota(jnp.int32, (tokens, tokens), 0) >= lax.broadcasted_iota(jnp.int32, (tokens, tokens), 1)
        rank = jnp.dot(jnp.where(before, 1.0, 0.0).astype(jnp.bfloat16), member.astype(jnp.bfloat16), preferred_element_type=jnp.float32)
        slot = jnp.where(member > 0.0, rank - 1.0, -1.0)
        load.wait()
        logits = jnp.dot(xv[...], w_ref[...], preferred_element_type=jnp.float32)
        top = jnp.max(logits, axis=-1, keepdims=True)
        ex = jnp.exp(logits - top)
        gates = ROUTE_SCALE * (ex / jnp.sum(ex, axis=-1, keepdims=True)) * member
        pad = jnp.zeros((tokens, LANES - experts), jnp.float32)
        slot_t[...] = jnp.transpose(jnp.concatenate([slot, pad], axis=1))[:experts]
        gt = jnp.transpose(jnp.concatenate([gates, pad], axis=1))[:experts]
        g1 = gt.astype(jnp.bfloat16).astype(jnp.float32)
        g2 = (gt - g1).astype(jnp.bfloat16).astype(jnp.float32)
        g3 = (gt - g1 - g2).astype(jnp.bfloat16).astype(jnp.float32)
        parts_t[0] = g1
        parts_t[1] = g2
        parts_t[2] = g3
        col = lax.broadcasted_iota(jnp.int32, (8, tokens), 1)
        row = lax.broadcasted_iota(jnp.int32, (8, tokens), 0)
        base = jnp.where(row == 0, (col // 32).astype(jnp.float32), jnp.where(row == 1, (col % 32).astype(jnp.float32), jnp.where(row == 2, 1.0, 0.0)))
        want = lax.broadcasted_iota(jnp.int32, (width, tokens), 0).astype(jnp.float32)

        spare = (tokens + lax.broadcasted_iota(jnp.int32, (1, width), 1) % SPARE).astype(jnp.float32)

        @pl.loop(0, experts // unroll)
        def _(i):
            for u in range(unroll):
                e = i * unroll + u
                onehot = jnp.where(slot_t[pl.ds(e, 1), :] == want, 1.0, 0.0).astype(jnp.bfloat16)
                vrows = base
                for q in range(3):
                    vrows = jnp.where(row == 3 + q, parts_t[q, pl.ds(e, 1), :], vrows)
                res = lax.dot_general(vrows.astype(jnp.bfloat16), onehot, (((1,), (1,)), ((), ())), preferred_element_type=jnp.float32)
                tok = jnp.where(res[2:3] > 0.5, res[0:1] * 32.0 + res[1:2], spare)
                tok_ref[pl.ds(e, 1), :] = tok
                gate_ref[pl.ds(e, 1), :] = (res[5:6] + res[4:5]) + res[3:4]

    vmem = pl.BlockSpec(memory_space=pltpu.VMEM)
    return pl.pallas_call(
        kernel,
        out_shape=[jax.ShapeDtypeStruct((experts, width), jnp.float32)] * 2,
        in_specs=[pl.BlockSpec(memory_space=pl.ANY)] + [vmem] * 3,
        out_specs=[vmem] * 2,
        scratch_shapes=[
            pltpu.VMEM((experts, tokens), jnp.float32),
            pltpu.VMEM((3, experts, tokens), jnp.float32),
            pltpu.VMEM(hidden.shape, hidden.dtype),
            pltpu.SemaphoreType.DMA,
        ],
        compiler_params=pltpu.CompilerParams(vmem_limit_bytes=48 * 1024 * 1024),
        cost_estimate=pl.CostEstimate(flops=20_000_000_000, bytes_accessed=8_000_000, transcendentals=100_000),
    )(hidden, w_router, top_idx, keep_mask)


def split(n, parts):
    return [(n * i // parts, n * (i + 1) // parts) for i in range(parts)]


def expert_pass(ids, xa, xb, tok, gate, w1, w3, w2, cap, b_dtype):
    T, C, L = xa.shape
    E, D, F = w1.shape
    M = 2 * cap
    S = M + 1
    nU, nD = F // 128, D // 256
    base = 2 * (T + SPARE) * C
    mark = -(-(base + C * S) // 8) * 8
    narrow = b_dtype == jnp.bfloat16

    def kernel(ids_ref, tok_all, gate_all, xa_ref, xb_ref, w1_ref, w3_ref, w2_ref, oa_ref, ob_ref,
               xv, mem, w1v, w3v, w2v, g, av, tok_ref, gate_ref, xsem, wsem, osem, tsem):
        first = [0, E]
        lists = [pltpu.make_async_copy(src.at[pl.ds(pl.multiple_of(ids_ref[b] * E, E), E)], dst.at[pl.ds(b * E, E)], tsem.at[b, i]) for b in range(2) for i, (src, dst) in enumerate(((tok_all, tok_ref), (gate_all, gate_ref)))]
        for c in lists: c.start()
        x_refs = (xa_ref, xb_ref)

        def weights(e, p):
            return [pltpu.make_async_copy(src.at[e], dst.at[p], wsem.at[p, i]) for i, (src, dst) in enumerate(((w1_ref, w1v), (w3_ref, w3v), (w2_ref, w2v)))]

        def spread(e, b, c):
            t = tok_ref[first[b] + e, c] + b * (T + SPARE)
            mem[pl.ds(base + b * cap + c, C, stride=S), :] = xv[t].astype(jnp.float32)

        def convert(j):
            g[j] = mem[base + j * S:base + j * S + M, :].astype(jnp.bfloat16)

        def scatter(e, b, cols):
            vals = []
            for c in cols:
                t = tok_ref[first[b] + e, c] + b * (T + SPARE)
                at = pl.ds(pl.multiple_of(t * C, C), C)
                vals.append((at, mem[at, :] + gate_ref[first[b] + e, c] * mem[pl.ds(base + b * cap + c, C, stride=S), :]))
            for at, v in vals:
                mem[at, :] = v

        loads = [pltpu.make_async_copy(x_refs[b], xv.at[pl.ds(b * (T + SPARE), T)], xsem.at[b]) for b in range(2)]
        for c in loads: c.start()
        for c in weights(0, 0): c.start(priority=1)
        for b in range(2):
            for k in range(SPARE):
                xv[b * (T + SPARE) + T + k] = jnp.zeros((C, L), xv.dtype)

        @pl.loop(0, 2 * (T + SPARE) // 16)
        def _(i):
            mem[pl.ds(pl.multiple_of(i * 16 * C, 8), 16 * C), :] = jnp.zeros((16 * C, L), jnp.float32)

        for c in lists: c.wait()
        for b in range(2):
            loads[b].wait()

            @pl.loop(0, cap // 16)
            def _(i):
                for u in range(16):
                    spread(0, b, i * 16 + u)
        for j in range(C): convert(j)

        @pl.loop(0, C)
        def _(i):
            mem[pl.ds(base + i * S, S), :] = jnp.zeros((S, L), jnp.float32)

        def up_tile(p, n, lo, hi):
            cols = pl.ds(n * L, L)
            rows = jnp.concatenate([g[j, lo:hi] for j in range(C)], axis=1)
            h = jnp.dot(rows, jnp.concatenate([w1v[p, :, cols], w3v[p, :, cols]], axis=1), preferred_element_type=jnp.float32)
            av[n, lo:hi] = (jax.nn.silu(h[:, :L]) * h[:, L:]).astype(jnp.bfloat16)
            mem[pl.ds(mark, 8), :] = h[:8, :L]

        def down_tile(p, n):
            act = jnp.concatenate([av[j] for j in range(nU)], axis=1)
            h = jnp.dot(act, w2v[p, :, pl.ds(n * 256, 256)], preferred_element_type=jnp.float32)
            h = h.astype(jnp.bfloat16).astype(jnp.float32)
            for k in range(2):
                mem[pl.ds(base + (2 * n + k) * S, M), :] = h[:, L * k:L * k + L]

        rows_of = [(b, c) for b in range(2) for c in range(cap)]
        parts = split(M, 2 * nU)

        @pl.loop(0, E)
        def _(e):
            p = lax.rem(e, 2)
            prev = jnp.maximum(e - 1, 0)
            ahead = jnp.minimum(e + 1, E - 1)
            for c in weights(e, p): c.wait()

            @pl.when(e + 1 < E)
            def _():
                for c in weights(e + 1, 1 - p): c.start(priority=1)

            for n in range(nU):
                for q in range(2):
                    for b, c in rows_of[slice(*parts[2 * n + q])]:
                        scatter(prev, b, [c])
                        spread(ahead, b, c)
                    up_tile(p, n, q * M // 2, (q + 1) * M // 2)
            for n in range(nD):
                convert(2 * n)
                convert(2 * n + 1)
                down_tile(p, n)

        def out(b):
            if b and narrow:
                return pltpu.make_async_copy(xv.at[pl.ds(0, T)], ob_ref, osem.at[b])
            return pltpu.make_async_copy(mem.at[pl.ds(b * (T + SPARE) * C, T * C)], (oa_ref, ob_ref)[b], osem.at[b])

        for b in range(2):
            @pl.loop(0, cap // 8)
            def _(i):
                scatter(E - 1, b, [i * 8 + u for u in range(8)])

            if b and narrow:
                @pl.loop(0, T // 8)
                def _(i):
                    for u in range(8):
                        r = i * 8 + u
                        xv[r] = mem[pl.ds(pl.multiple_of((T + SPARE + r) * C, C), C), :].astype(b_dtype)
            out(b).start()
        for b in range(2):
            out(b).wait()

    anyspec = pl.BlockSpec(memory_space=pl.ANY)
    smem = pl.BlockSpec(memory_space=pltpu.SMEM)
    rows = E * M
    return pl.pallas_call(
        kernel,
        out_shape=[jax.ShapeDtypeStruct((T * C, L), jnp.float32), jax.ShapeDtypeStruct((T, C, L) if narrow else (T * C, L), b_dtype)],
        in_specs=[smem] + [anyspec] * 7,
        out_specs=[anyspec] * 2,
        scratch_shapes=[
            pltpu.VMEM((2 * (T + SPARE), C, L), jnp.bfloat16),
            pltpu.VMEM((mark + 8, L), jnp.float32),
            pltpu.VMEM((2, D, F), jnp.bfloat16), pltpu.VMEM((2, D, F), jnp.bfloat16), pltpu.VMEM((2, F, D), jnp.bfloat16),
            pltpu.VMEM((C, M, L), jnp.bfloat16),
            pltpu.VMEM((nU, M, L), jnp.bfloat16),
            pltpu.SMEM((2 * E, tok.shape[1]), jnp.int32), pltpu.SMEM((2 * E, tok.shape[1]), jnp.float32),
            pltpu.SemaphoreType.DMA((2,)), pltpu.SemaphoreType.DMA((2, 3)), pltpu.SemaphoreType.DMA((2,)), pltpu.SemaphoreType.DMA((2, 2)),
        ],
        compiler_params=pltpu.CompilerParams(vmem_limit_bytes=67000000),
        cost_estimate=pl.CostEstimate(flops=rows * D * F * 6, bytes_accessed=E * D * F * 6, transcendentals=rows * F),
    )(ids, tok, gate, xa, xb, w1, w3, w2)


def shared_rows(hidden, gate_w, up_w, down_w, total, row0, rows):
    tokens, width = hidden.shape
    ff = gate_w.shape[1]
    tile = 256
    n_up, n_down = ff // tile, width // tile
    up_parts, down_parts = split(n_up, 4), split(n_down, 2)

    def kernel(x_ref, g_ref, u_ref, d_ref, *rest):
        out_ref, xv, gv, uv, dv, act, yv, sem, usem, dsem, osem = rest[-11:]
        load_x = pltpu.make_async_copy(x_ref.at[pl.ds(row0, rows)], xv, sem)
        load_x.start()

        def up_loads(i):
            cols = pl.ds(up_parts[i][0] * tile, (up_parts[i][1] - up_parts[i][0]) * tile)
            return [pltpu.make_async_copy(src.at[:, cols], dst.at[:, cols], usem.at[i, k]) for k, (src, dst) in enumerate(((g_ref, gv), (u_ref, uv)))]

        def down_loads(i):
            cols = pl.ds(down_parts[i][0] * tile, (down_parts[i][1] - down_parts[i][0]) * tile)
            return pltpu.make_async_copy(d_ref.at[:, cols], dv.at[:, cols], dsem.at[i])

        chunks = [up_loads(i) for i in range(len(up_parts))] + [[down_loads(i)] for i in range(len(down_parts))]

        def begin(i):
            if i < len(chunks):
                for c in chunks[i]:
                    c.start()

        def arrive(i):
            for c in chunks[i]:
                c.wait()
            begin(i + 2)

        begin(0)
        load_x.wait()
        begin(1)
        for i, (lo, hi) in enumerate(up_parts):
            arrive(i)
            for n in range(lo, hi):
                cols = slice(n * tile, (n + 1) * tile)
                h_gate = jnp.dot(xv[...], gv[:, cols], preferred_element_type=jnp.float32)
                h_up = jnp.dot(xv[...], uv[:, cols], preferred_element_type=jnp.float32)
                act[:, cols] = (jax.nn.silu(h_gate) * h_up).astype(jnp.bfloat16)

        def store(i):
            cols = pl.ds(down_parts[i][0] * tile, (down_parts[i][1] - down_parts[i][0]) * tile)
            return pltpu.make_async_copy(yv.at[:, cols], out_ref.at[pl.ds(row0, rows), cols], osem.at[i])

        for i, (lo, hi) in enumerate(down_parts):
            arrive(len(up_parts) + i)
            for n in range(lo, hi):
                cols = slice(n * tile, (n + 1) * tile)
                yv[:, cols] = jnp.dot(act[...], dv[:, cols], preferred_element_type=jnp.float32)
            store(i).start()
        for i in range(len(down_parts)):
            store(i).wait()

    operands = [hidden, gate_w, up_w, down_w] + ([] if total is None else [total])
    anyspec = pl.BlockSpec(memory_space=pl.ANY)
    return pl.pallas_call(
        kernel,
        out_shape=jax.ShapeDtypeStruct((tokens, width), jnp.float32),
        in_specs=[anyspec] * len(operands),
        out_specs=anyspec,
        scratch_shapes=[
            pltpu.VMEM((rows, width), jnp.bfloat16),
            pltpu.VMEM((width, ff), jnp.bfloat16), pltpu.VMEM((width, ff), jnp.bfloat16), pltpu.VMEM((ff, width), jnp.bfloat16),
            pltpu.VMEM((rows, ff), jnp.bfloat16), pltpu.VMEM((rows, width), jnp.float32),
            pltpu.SemaphoreType.DMA, pltpu.SemaphoreType.DMA((len(up_parts), 2)), pltpu.SemaphoreType.DMA((len(down_parts),)), pltpu.SemaphoreType.DMA((len(down_parts),)),
        ],
        input_output_aliases={} if total is None else {4: 0},
        compiler_params=pltpu.CompilerParams(vmem_limit_bytes=67000000),
        cost_estimate=pl.CostEstimate(flops=rows * width * ff * 6, bytes_accessed=width * ff * 6, transcendentals=rows * ff),
    )(*operands)


def finish(shared, pa, q, r1, r2, r3):
    tokens, width = shared.shape
    n, depth = 16, 6
    rows = tokens // n
    C = width // LANES
    S = rows + 1

    def kernel(ys_ref, pa_ref, q_ref, r1_ref, r2_ref, r3_ref, out_ref, yv, pv, rv, ov, buf, lsem, osem):
        def loads(i):
            part = pl.ds(i * rows, rows)
            copies = [(ys_ref.at[part], yv.at[part]), (pa_ref.at[part], pv.at[part])]
            copies += [(src.at[part], rv.at[k, part]) for k, src in enumerate((q_ref, r1_ref, r2_ref, r3_ref))]
            return [pltpu.make_async_copy(src, dst, lsem.at[i, k]) for k, (src, dst) in enumerate(copies)]

        def store(i):
            part = pl.ds(i * rows, rows)
            return pltpu.make_async_copy(ov.at[part], out_ref.at[part], osem.at[i])

        for i in range(depth):
            for c in loads(i): c.start()
        for i in range(n):
            for c in loads(i): c.wait()
            if i + depth < n:
                for c in loads(i + depth): c.start()

            @pl.loop(0, rows // 8)
            def _(k):
                for u in range(8):
                    r = i * rows + k * 8 + u
                    v = pv[r]
                    for t in range(4):
                        v = v + rv[t, r].astype(jnp.float32)
                    buf[pl.ds(k * 8 + u, C, stride=S), :] = v

            for j in range(C):
                at, cols = slice(i * rows, (i + 1) * rows), slice(j * LANES, (j + 1) * LANES)
                ov[at, cols] = (yv[at, cols] + buf[j * S:j * S + rows, :]).astype(jnp.bfloat16)
            store(i).start()
        for i in range(n):
            store(i).wait()

    anyspec = pl.BlockSpec(memory_space=pl.ANY)
    return pl.pallas_call(
        kernel,
        out_shape=jax.ShapeDtypeStruct((tokens, width), jnp.bfloat16),
        in_specs=[anyspec] * 6,
        out_specs=anyspec,
        scratch_shapes=[
            pltpu.VMEM((tokens, width), jnp.float32), pltpu.VMEM(pa.shape, jnp.float32), pltpu.VMEM((4,) + q.shape, jnp.bfloat16),
            pltpu.VMEM((tokens, width), jnp.bfloat16), pltpu.VMEM((C * S, LANES), jnp.float32),
            pltpu.SemaphoreType.DMA((n, 6)), pltpu.SemaphoreType.DMA((n,)),
        ],
        compiler_params=pltpu.CompilerParams(vmem_limit_bytes=67000000),
        cost_estimate=pl.CostEstimate(flops=tokens * width * 6, bytes_accessed=tokens * width * 20, transcendentals=0),
    )(shared, pa, q, r1, r2, r3)


def add_partials(pa, q):
    tokens, C, L = pa.shape
    n, depth = 16, 10
    rows = tokens // n

    def kernel(a_ref, q_ref, out_ref, av, qv, cv, asem, qsem, csem):
        part = [pl.ds(i * rows, rows) for i in range(n)]

        def loads(i):
            return [pltpu.make_async_copy(a_ref.at[part[i]], av.at[part[i]], asem.at[i]), pltpu.make_async_copy(q_ref.at[part[i]], qv.at[part[i]], qsem.at[i])]

        def store(i):
            return pltpu.make_async_copy(cv.at[part[i]], out_ref.at[part[i]], csem.at[i])

        for i in range(depth):
            for c in loads(i): c.start()
        for i in range(n):
            for c in loads(i): c.wait()
            if i + depth < n:
                for c in loads(i + depth): c.start()

            @pl.loop(0, rows // 8)
            def _(k):
                at = pl.ds(i * rows + k * 8, 8)
                cv[at] = (av[at] + qv[at]).astype(jnp.bfloat16)

            store(i).start()
        for i in range(n):
            store(i).wait()

    anyspec = pl.BlockSpec(memory_space=pl.ANY)
    return pl.pallas_call(
        kernel,
        out_shape=jax.ShapeDtypeStruct(pa.shape, jnp.bfloat16),
        in_specs=[anyspec] * 2,
        out_specs=anyspec,
        scratch_shapes=[
            pltpu.VMEM(pa.shape, jnp.float32), pltpu.VMEM(pa.shape, jnp.float32), pltpu.VMEM(pa.shape, jnp.bfloat16),
            pltpu.SemaphoreType.DMA((n,)), pltpu.SemaphoreType.DMA((n,)), pltpu.SemaphoreType.DMA((n,)),
        ],
        compiler_params=pltpu.CompilerParams(vmem_limit_bytes=67000000),
        cost_estimate=pl.CostEstimate(flops=tokens * C * L, bytes_accessed=tokens * C * L * 10, transcendentals=0),
    )(pa, q)


def after(value, *deps):
    return lax.optimization_barrier((value, deps))[0]


def solution(mesh):
    n_dev = mesh.shape["ep"]
    chips = n_dev // 2
    tok_spec = P(("dp", "ep"), None)
    bank_spec = P("ep", None, None)
    near = [(2 * c + k, 2 * ((c + (-1 if k == 0 else 1)) % chips) + k) for c in range(chips) for k in range(2)]
    far = [(d, s) for s, d in near]
    across = [(2 * c + k, 2 * ((c + 2) % chips) + k) for c in range(chips) for k in range(2)]
    swap = [(2 * c + k, 2 * c + 1 - k) for c in range(chips) for k in range(2)]

    def device_fn(hidden, w_router, w_gate, w_up, w_down, shared_gate, shared_up, shared_down, top_idx, keep_mask):
        tokens, top_k = top_idx.shape
        width = hidden.shape[1]
        experts = w_router.shape[1]
        per_dev = w_gate.shape[0]
        cap = 8 * ((top_k * tokens + 4 * experts - 1) // (4 * experts))
        me = lax.axis_index("ep")
        chip, core = me // 2, me % 2

        def perm(v, p):
            return lax.ppermute(v, "ep", p)

        x0 = hidden.reshape(tokens, width // LANES, LANES)
        x1 = perm(x0, near)
        tok, gate = route_tables(after(hidden, x0), w_router, top_idx, keep_mask, cap)
        table = jnp.stack([tok, gate], axis=0).reshape(2, n_dev, per_dev, tok.shape[1])
        table = lax.all_to_all(table, "ep", 1, 1, tiled=False)
        table = table.reshape(2, experts, tok.shape[1])
        tok_all, gate_all = table[0].astype(jnp.int32), table[1]

        def shared_piece(total, dep, lo, hi):
            return shared_rows(after(hidden, dep), shared_gate, shared_up, shared_down, total, lo * tokens // 4, (hi - lo) * tokens // 4)

        x0s = perm(x0, swap)
        x1s = perm(x1, swap)
        x3 = perm(x1, near)
        x3s = perm(x3, swap)

        dirn = jnp.where(core == 0, 1, -1)

        def src(off, k):
            return 2 * ((chip + off + chips) % chips) + k

        def one_pass(xa, xb, off_a, off_b, b_dtype=jnp.float32):
            ids = jnp.stack([src(off_a, core), src(off_b, 1 - core)]).astype(jnp.int32)
            sums = expert_pass(ids, xa, xb, tok_all, gate_all, w_gate, w_up, w_down, cap, b_dtype)
            return [v.reshape(xa.shape) for v in sums]

        def add(pa, q, dep):
            return add_partials(after(pa, dep), q)

        y = shared_piece(None, tok, 0, 2)
        pa1, pb1 = one_pass(after(x1, y, x1s), x1s, dirn, -dirn)
        x2 = perm(after(x0, pa1), far)
        x2s = perm(x2, swap)
        q1 = perm(pb1, swap)
        pa2, pb2 = one_pass(after(x3, pa1), x3s, 2, 2)
        q2 = perm(pb2, swap)
        c1 = add(pa1, q1, pa2)
        r1 = perm(c1, far)
        c2 = add(pa2, q2, c1)
        r2 = perm(c2, across)
        pa3, pb3 = one_pass(after(x2, c2), x2s, -dirn, dirn)
        q3 = perm(pb3, swap)
        y = shared_piece(y, pa3, 2, 3)
        c3 = add(pa3, q3, y)
        r3 = perm(c3, near)
        pa4, pb4 = one_pass(after(x0, c3), x0s, 0, 0, jnp.bfloat16)
        q4 = perm(pb4, swap)
        y = shared_piece(y, (pa4, pb4), 3, 4)
        return finish(y, pa4, q4, r1, r2, r3)

    return jax.shard_map(device_fn, mesh=mesh, in_specs=(tok_spec, P(), bank_spec, bank_spec, bank_spec, P(), P(), P(), tok_spec, tok_spec), out_specs=tok_spec, check_vma=False)
```

```python
import jax
import jax.numpy as jnp
from jax import lax
from jax.experimental import pallas as pl
from jax.experimental.pallas import tpu as pltpu
from jax.sharding import PartitionSpec as P


ROUTE_SCALE = 16.0
LANES = 128
SPARE = 8


def route_tables(hidden, w_router, top_idx, keep_mask, cap):
    tokens, top_k = top_idx.shape
    experts = w_router.shape[1]
    width, unroll = cap, 4

    def kernel(x_ref, w_ref, idx_ref, keep_ref, tok_ref, gate_ref, slot_t, parts_t, xv, sem):
        load = pltpu.make_async_copy(x_ref, xv, sem)
        load.start()
        lane = lax.broadcasted_iota(jnp.int32, (tokens, experts), 1)
        member = jnp.zeros((tokens, experts), jnp.float32)
        for k in range(top_k):
            hit = (idx_ref[:, k:k + 1] == lane) & (keep_ref[:, k:k + 1] > 0)
            member = jnp.where(hit, 1.0, member)
        before = lax.broadcasted_iota(jnp.int32, (tokens, tokens), 0) >= lax.broadcasted_iota(jnp.int32, (tokens, tokens), 1)
        rank = jnp.dot(jnp.where(before, 1.0, 0.0).astype(jnp.bfloat16), member.astype(jnp.bfloat16), preferred_element_type=jnp.float32)
        slot = jnp.where(member > 0.0, rank - 1.0, -1.0)
        load.wait()
        logits = jnp.dot(xv[...], w_ref[...], preferred_element_type=jnp.float32)
        top = jnp.max(logits, axis=-1, keepdims=True)
        ex = jnp.exp(logits - top)
        gates = ROUTE_SCALE * (ex / jnp.sum(ex, axis=-1, keepdims=True)) * member
        pad = jnp.zeros((tokens, LANES - experts), jnp.float32)
        slot_t[...] = jnp.transpose(jnp.concatenate([slot, pad], axis=1))[:experts]
        gt = jnp.transpose(jnp.concatenate([gates, pad], axis=1))[:experts]
        g1 = gt.astype(jnp.bfloat16).astype(jnp.float32)
        g2 = (gt - g1).astype(jnp.bfloat16).astype(jnp.float32)
        g3 = (gt - g1 - g2).astype(jnp.bfloat16).astype(jnp.float32)
        parts_t[0] = g1
        parts_t[1] = g2
        parts_t[2] = g3
        col = lax.broadcasted_iota(jnp.int32, (8, tokens), 1)
        row = lax.broadcasted_iota(jnp.int32, (8, tokens), 0)
        base = jnp.where(row == 0, (col // 32).astype(jnp.float32), jnp.where(row == 1, (col % 32).astype(jnp.float32), jnp.where(row == 2, 1.0, 0.0)))
        want = lax.broadcasted_iota(jnp.int32, (width, tokens), 0).astype(jnp.float32)

        spare = (tokens + lax.broadcasted_iota(jnp.int32, (1, width), 1) % SPARE).astype(jnp.float32)

        @pl.loop(0, experts // unroll)
        def _(i):
            for u in range(unroll):
                e = i * unroll + u
                onehot = jnp.where(slot_t[pl.ds(e, 1), :] == want, 1.0, 0.0).astype(jnp.bfloat16)
                vrows = base
                for q in range(3):
                    vrows = jnp.where(row == 3 + q, parts_t[q, pl.ds(e, 1), :], vrows)
                res = lax.dot_general(vrows.astype(jnp.bfloat16), onehot, (((1,), (1,)), ((), ())), preferred_element_type=jnp.float32)
                tok = jnp.where(res[2:3] > 0.5, res[0:1] * 32.0 + res[1:2], spare)
                tok_ref[pl.ds(e, 1), :] = tok
                gate_ref[pl.ds(e, 1), :] = (res[5:6] + res[4:5]) + res[3:4]

    vmem = pl.BlockSpec(memory_space=pltpu.VMEM)
    return pl.pallas_call(
        kernel,
        out_shape=[jax.ShapeDtypeStruct((experts, width), jnp.float32)] * 2,
        in_specs=[pl.BlockSpec(memory_space=pl.ANY)] + [vmem] * 3,
        out_specs=[vmem] * 2,
        scratch_shapes=[
            pltpu.VMEM((experts, tokens), jnp.float32),
            pltpu.VMEM((3, experts, tokens), jnp.float32),
            pltpu.VMEM(hidden.shape, hidden.dtype),
            pltpu.SemaphoreType.DMA,
        ],
        compiler_params=pltpu.CompilerParams(vmem_limit_bytes=48 * 1024 * 1024),
        cost_estimate=pl.CostEstimate(flops=20_000_000_000, bytes_accessed=8_000_000, transcendentals=100_000),
    )(hidden, w_router, top_idx, keep_mask)


def split(n, parts):
    return [(n * i // parts, n * (i + 1) // parts) for i in range(parts)]


def expert_pass(ids, xa, xb, tok, gate, w1, w3, w2, cap, b_dtype):
    T, C, L = xa.shape
    E, D, F = w1.shape
    M = 2 * cap
    S = M + 1
    nU, nD = F // 128, D // 256
    base = 2 * (T + SPARE) * C
    mark = -(-(base + C * S) // 8) * 8
    narrow = b_dtype == jnp.bfloat16

    def kernel(ids_ref, tok_all, gate_all, xa_ref, xb_ref, w1_ref, w3_ref, w2_ref, oa_ref, ob_ref,
               xv, mem, w1v, w3v, w2v, g, av, tok_ref, gate_ref, xsem, wsem, osem, tsem):
        first = [0, E]
        lists = [pltpu.make_async_copy(src.at[pl.ds(pl.multiple_of(ids_ref[b] * E, E), E)], dst.at[pl.ds(b * E, E)], tsem.at[b, i]) for b in range(2) for i, (src, dst) in enumerate(((tok_all, tok_ref), (gate_all, gate_ref)))]
        for c in lists: c.start()
        x_refs = (xa_ref, xb_ref)

        def weights(e, p):
            return [pltpu.make_async_copy(src.at[e], dst.at[p], wsem.at[p, i]) for i, (src, dst) in enumerate(((w1_ref, w1v), (w3_ref, w3v), (w2_ref, w2v)))]

        def spread(e, b, c):
            t = tok_ref[first[b] + e, c] + b * (T + SPARE)
            mem[pl.ds(base + b * cap + c, C, stride=S), :] = xv[t].astype(jnp.float32)

        def convert(j):
            g[j] = mem[base + j * S:base + j * S + M, :].astype(jnp.bfloat16)

        def scatter(e, b, cols):
            vals = []
            for c in cols:
                t = tok_ref[first[b] + e, c] + b * (T + SPARE)
                at = pl.ds(pl.multiple_of(t * C, C), C)
                vals.append((at, mem[at, :] + gate_ref[first[b] + e, c] * mem[pl.ds(base + b * cap + c, C, stride=S), :]))
            for at, v in vals:
                mem[at, :] = v

        loads = [pltpu.make_async_copy(x_refs[b], xv.at[pl.ds(b * (T + SPARE), T)], xsem.at[b]) for b in range(2)]
        for c in loads: c.start()
        for c in weights(0, 0): c.start(priority=1)
        for b in range(2):
            for k in range(SPARE):
                xv[b * (T + SPARE) + T + k] = jnp.zeros((C, L), xv.dtype)

        @pl.loop(0, 2 * (T + SPARE) // 16)
        def _(i):
            mem[pl.ds(pl.multiple_of(i * 16 * C, 8), 16 * C), :] = jnp.zeros((16 * C, L), jnp.float32)

        for c in lists: c.wait()
        for b in range(2):
            loads[b].wait()

            @pl.loop(0, cap // 16)
            def _(i):
                for u in range(16):
                    spread(0, b, i * 16 + u)
        for j in range(C): convert(j)

        @pl.loop(0, C)
        def _(i):
            mem[pl.ds(base + i * S, S), :] = jnp.zeros((S, L), jnp.float32)

        def up_tile(p, n, lo, hi):
            cols = pl.ds(n * L, L)
            rows = jnp.concatenate([g[j, lo:hi] for j in range(C)], axis=1)
            h = jnp.dot(rows, jnp.concatenate([w1v[p, :, cols], w3v[p, :, cols]], axis=1), preferred_element_type=jnp.float32)
            av[n, lo:hi] = (jax.nn.silu(h[:, :L]) * h[:, L:]).astype(jnp.bfloat16)
            mem[pl.ds(mark, 8), :] = h[:8, :L]

        def down_tile(p, n, lo, hi):
            act = jnp.concatenate([av[j, lo:hi] for j in range(nU)], axis=1)
            h = jnp.dot(act, w2v[p, :, pl.ds(n * 256, 256)], preferred_element_type=jnp.float32)
            h = h.astype(jnp.bfloat16).astype(jnp.float32)
            for k in range(2):
                mem[pl.ds(base + (2 * n + k) * S + lo, hi - lo), :] = h[:, L * k:L * k + L]

        rows_of = [(b, c) for b in range(2) for c in range(cap)]
        parts = split(M, 2 * nU)

        @pl.loop(0, E)
        def _(e):
            p = lax.rem(e, 2)
            prev = jnp.maximum(e - 1, 0)
            ahead = jnp.minimum(e + 1, E - 1)
            for c in weights(e, p): c.wait()

            @pl.when(e + 1 < E)
            def _():
                for c in weights(e + 1, 1 - p): c.start(priority=1)

            for n in range(nU):
                for q in range(2):
                    for b, c in rows_of[slice(*parts[2 * n + q])]:
                        scatter(prev, b, [c])
                        spread(ahead, b, c)
                    up_tile(p, n, q * M // 2, (q + 1) * M // 2)
            for n in range(nD):
                convert(2 * n)
                convert(2 * n + 1)
                down_tile(p, n, 0, M // 2)
                down_tile(p, n, M // 2, M)

        def out(b):
            if b and narrow:
                return pltpu.make_async_copy(xv.at[pl.ds(0, T)], ob_ref, osem.at[b])
            return pltpu.make_async_copy(mem.at[pl.ds(b * (T + SPARE) * C, T * C)], (oa_ref, ob_ref)[b], osem.at[b])

        for b in range(2):
            @pl.loop(0, cap // 8)
            def _(i):
                scatter(E - 1, b, [i * 8 + u for u in range(8)])

            if b and narrow:
                @pl.loop(0, T // 8)
                def _(i):
                    for u in range(8):
                        r = i * 8 + u
                        xv[r] = mem[pl.ds(pl.multiple_of((T + SPARE + r) * C, C), C), :].astype(b_dtype)
            out(b).start()
        for b in range(2):
            out(b).wait()

    anyspec = pl.BlockSpec(memory_space=pl.ANY)
    smem = pl.BlockSpec(memory_space=pltpu.SMEM)
    rows = E * M
    return pl.pallas_call(
        kernel,
        out_shape=[jax.ShapeDtypeStruct((T * C, L), jnp.float32), jax.ShapeDtypeStruct((T, C, L) if narrow else (T * C, L), b_dtype)],
        in_specs=[smem] + [anyspec] * 7,
        out_specs=[anyspec] * 2,
        scratch_shapes=[
            pltpu.VMEM((2 * (T + SPARE), C, L), jnp.bfloat16),
            pltpu.VMEM((mark + 8, L), jnp.float32),
            pltpu.VMEM((2, D, F), jnp.bfloat16), pltpu.VMEM((2, D, F), jnp.bfloat16), pltpu.VMEM((2, F, D), jnp.bfloat16),
            pltpu.VMEM((C, M, L), jnp.bfloat16),
            pltpu.VMEM((nU, M, L), jnp.bfloat16),
            pltpu.SMEM((2 * E, tok.shape[1]), jnp.int32), pltpu.SMEM((2 * E, tok.shape[1]), jnp.float32),
            pltpu.SemaphoreType.DMA((2,)), pltpu.SemaphoreType.DMA((2, 3)), pltpu.SemaphoreType.DMA((2,)), pltpu.SemaphoreType.DMA((2, 2)),
        ],
        compiler_params=pltpu.CompilerParams(vmem_limit_bytes=67000000),
        cost_estimate=pl.CostEstimate(flops=rows * D * F * 6, bytes_accessed=E * D * F * 6, transcendentals=rows * F),
    )(ids, tok, gate, xa, xb, w1, w3, w2)


def shared_rows(hidden, gate_w, up_w, down_w, total, row0, rows):
    tokens, width = hidden.shape
    ff = gate_w.shape[1]
    tile = 256
    n_up, n_down = ff // tile, width // tile
    up_parts, down_parts = (split(n_up, 6), split(n_down, 4)) if 4 * rows <= tokens else (split(n_up, 4), split(n_down, 2))
    ahead = 3 if 4 * rows <= tokens else 2

    def kernel(x_ref, g_ref, u_ref, d_ref, *rest):
        out_ref, xv, gv, uv, dv, act, yv, sem, usem, dsem, osem = rest[-11:]
        load_x = pltpu.make_async_copy(x_ref.at[pl.ds(row0, rows)], xv, sem)
        load_x.start()

        def up_loads(i):
            cols = pl.ds(up_parts[i][0] * tile, (up_parts[i][1] - up_parts[i][0]) * tile)
            return [pltpu.make_async_copy(src.at[:, cols], dst.at[:, cols], usem.at[i, k]) for k, (src, dst) in enumerate(((g_ref, gv), (u_ref, uv)))]

        def down_loads(i):
            cols = pl.ds(down_parts[i][0] * tile, (down_parts[i][1] - down_parts[i][0]) * tile)
            return pltpu.make_async_copy(d_ref.at[:, cols], dv.at[:, cols], dsem.at[i])

        chunks = [up_loads(i) for i in range(len(up_parts))] + [[down_loads(i)] for i in range(len(down_parts))]

        def begin(i):
            if i < len(chunks):
                for c in chunks[i]:
                    c.start()

        def arrive(i):
            for c in chunks[i]:
                c.wait()
            begin(i + ahead)

        begin(0)
        load_x.wait()
        for i in range(1, ahead):
            begin(i)
        for i, (lo, hi) in enumerate(up_parts):
            arrive(i)
            for n in range(lo, hi):
                cols = slice(n * tile, (n + 1) * tile)
                h_gate = jnp.dot(xv[...], gv[:, cols], preferred_element_type=jnp.float32)
                h_up = jnp.dot(xv[...], uv[:, cols], preferred_element_type=jnp.float32)
                act[:, cols] = (jax.nn.silu(h_gate) * h_up).astype(jnp.bfloat16)

        def store(i):
            cols = pl.ds(down_parts[i][0] * tile, (down_parts[i][1] - down_parts[i][0]) * tile)
            return pltpu.make_async_copy(yv.at[:, cols], out_ref.at[pl.ds(row0, rows), cols], osem.at[i])

        for i, (lo, hi) in enumerate(down_parts):
            arrive(len(up_parts) + i)
            for n in range(lo, hi):
                cols = slice(n * tile, (n + 1) * tile)
                yv[:, cols] = jnp.dot(act[...], dv[:, cols], preferred_element_type=jnp.float32)
            store(i).start()
        for i in range(len(down_parts)):
            store(i).wait()

    operands = [hidden, gate_w, up_w, down_w] + ([] if total is None else [total])
    anyspec = pl.BlockSpec(memory_space=pl.ANY)
    return pl.pallas_call(
        kernel,
        out_shape=jax.ShapeDtypeStruct((tokens, width), jnp.float32),
        in_specs=[anyspec] * len(operands),
        out_specs=anyspec,
        scratch_shapes=[
            pltpu.VMEM((rows, width), jnp.bfloat16),
            pltpu.VMEM((width, ff), jnp.bfloat16), pltpu.VMEM((width, ff), jnp.bfloat16), pltpu.VMEM((ff, width), jnp.bfloat16),
            pltpu.VMEM((rows, ff), jnp.bfloat16), pltpu.VMEM((rows, width), jnp.float32),
            pltpu.SemaphoreType.DMA, pltpu.SemaphoreType.DMA((len(up_parts), 2)), pltpu.SemaphoreType.DMA((len(down_parts),)), pltpu.SemaphoreType.DMA((len(down_parts),)),
        ],
        input_output_aliases={} if total is None else {4: 0},
        compiler_params=pltpu.CompilerParams(vmem_limit_bytes=67000000),
        cost_estimate=pl.CostEstimate(flops=rows * width * ff * 6, bytes_accessed=width * ff * 6, transcendentals=rows * ff),
    )(*operands)


def finish(shared, pa, q, r1, r2, r3):
    tokens, width = shared.shape
    n, depth = 16, 6
    rows = tokens // n
    C = width // LANES
    S = rows + 1

    def kernel(ys_ref, pa_ref, q_ref, r1_ref, r2_ref, r3_ref, out_ref, yv, pv, rv, ov, buf, lsem, osem):
        def loads(i):
            part = pl.ds(i * rows, rows)
            copies = [(ys_ref.at[part], yv.at[part]), (pa_ref.at[part], pv.at[part])]
            copies += [(src.at[part], rv.at[k, part]) for k, src in enumerate((q_ref, r1_ref, r2_ref, r3_ref))]
            return [pltpu.make_async_copy(src, dst, lsem.at[i, k]) for k, (src, dst) in enumerate(copies)]

        def store(i):
            part = pl.ds(i * rows, rows)
            return pltpu.make_async_copy(ov.at[part], out_ref.at[part], osem.at[i])

        for i in range(depth):
            for c in loads(i): c.start()
        for i in range(n):
            for c in loads(i): c.wait()
            if i + depth < n:
                for c in loads(i + depth): c.start()

            @pl.loop(0, rows // 8)
            def _(k):
                for u in range(8):
                    r = i * rows + k * 8 + u
                    v = pv[r]
                    for t in range(4):
                        v = v + rv[t, r].astype(jnp.float32)
                    buf[pl.ds(k * 8 + u, C, stride=S), :] = v

            for j in range(C):
                at, cols = slice(i * rows, (i + 1) * rows), slice(j * LANES, (j + 1) * LANES)
                ov[at, cols] = (yv[at, cols] + buf[j * S:j * S + rows, :]).astype(jnp.bfloat16)
            store(i).start()
        for i in range(n):
            store(i).wait()

    anyspec = pl.BlockSpec(memory_space=pl.ANY)
    return pl.pallas_call(
        kernel,
        out_shape=jax.ShapeDtypeStruct((tokens, width), jnp.bfloat16),
        in_specs=[anyspec] * 6,
        out_specs=anyspec,
        scratch_shapes=[
            pltpu.VMEM((tokens, width), jnp.float32), pltpu.VMEM(pa.shape, jnp.float32), pltpu.VMEM((4,) + q.shape, jnp.bfloat16),
            pltpu.VMEM((tokens, width), jnp.bfloat16), pltpu.VMEM((C * S, LANES), jnp.float32),
            pltpu.SemaphoreType.DMA((n, 6)), pltpu.SemaphoreType.DMA((n,)),
        ],
        compiler_params=pltpu.CompilerParams(vmem_limit_bytes=67000000),
        cost_estimate=pl.CostEstimate(flops=tokens * width * 6, bytes_accessed=tokens * width * 20, transcendentals=0),
    )(shared, pa, q, r1, r2, r3)


def add_partials(pa, q):
    tokens, C, L = pa.shape
    n, depth = 16, 10
    rows = tokens // n

    def kernel(a_ref, q_ref, out_ref, av, qv, cv, asem, qsem, csem):
        part = [pl.ds(i * rows, rows) for i in range(n)]

        def loads(i):
            return [pltpu.make_async_copy(a_ref.at[part[i]], av.at[part[i]], asem.at[i]), pltpu.make_async_copy(q_ref.at[part[i]], qv.at[part[i]], qsem.at[i])]

        def store(i):
            return pltpu.make_async_copy(cv.at[part[i]], out_ref.at[part[i]], csem.at[i])

        for i in range(depth):
            for c in loads(i): c.start()
        for i in range(n):
            for c in loads(i): c.wait()
            if i + depth < n:
                for c in loads(i + depth): c.start()

            @pl.loop(0, rows // 8)
            def _(k):
                at = pl.ds(i * rows + k * 8, 8)
                cv[at] = (av[at] + qv[at]).astype(jnp.bfloat16)

            store(i).start()
        for i in range(n):
            store(i).wait()

    anyspec = pl.BlockSpec(memory_space=pl.ANY)
    return pl.pallas_call(
        kernel,
        out_shape=jax.ShapeDtypeStruct(pa.shape, jnp.bfloat16),
        in_specs=[anyspec] * 2,
        out_specs=anyspec,
        scratch_shapes=[
            pltpu.VMEM(pa.shape, jnp.float32), pltpu.VMEM(pa.shape, jnp.float32), pltpu.VMEM(pa.shape, jnp.bfloat16),
            pltpu.SemaphoreType.DMA((n,)), pltpu.SemaphoreType.DMA((n,)), pltpu.SemaphoreType.DMA((n,)),
        ],
        compiler_params=pltpu.CompilerParams(vmem_limit_bytes=67000000),
        cost_estimate=pl.CostEstimate(flops=tokens * C * L, bytes_accessed=tokens * C * L * 10, transcendentals=0),
    )(pa, q)


def after(value, *deps):
    return lax.optimization_barrier((value, deps))[0]


def solution(mesh):
    n_dev = mesh.shape["ep"]
    chips = n_dev // 2
    tok_spec = P(("dp", "ep"), None)
    bank_spec = P("ep", None, None)
    near = [(2 * c + k, 2 * ((c + (-1 if k == 0 else 1)) % chips) + k) for c in range(chips) for k in range(2)]
    far = [(d, s) for s, d in near]
    across = [(2 * c + k, 2 * ((c + 2) % chips) + k) for c in range(chips) for k in range(2)]
    swap = [(2 * c + k, 2 * c + 1 - k) for c in range(chips) for k in range(2)]

    def device_fn(hidden, w_router, w_gate, w_up, w_down, shared_gate, shared_up, shared_down, top_idx, keep_mask):
        tokens, top_k = top_idx.shape
        width = hidden.shape[1]
        experts = w_router.shape[1]
        per_dev = w_gate.shape[0]
        cap = 8 * ((top_k * tokens + 4 * experts - 1) // (4 * experts))
        me = lax.axis_index("ep")
        chip, core = me // 2, me % 2

        def perm(v, p):
            return lax.ppermute(v, "ep", p)

        x0 = hidden.reshape(tokens, width // LANES, LANES)
        x1 = perm(x0, near)
        tok, gate = route_tables(after(hidden, x0), w_router, top_idx, keep_mask, cap)
        table = jnp.stack([tok, gate], axis=0).reshape(2, n_dev, per_dev, tok.shape[1])
        table = lax.all_to_all(table, "ep", 1, 1, tiled=False)
        table = table.reshape(2, experts, tok.shape[1])
        tok_all, gate_all = table[0].astype(jnp.int32), table[1]

        def shared_piece(total, dep, lo, hi):
            return shared_rows(after(hidden, dep), shared_gate, shared_up, shared_down, total, lo * tokens // 4, (hi - lo) * tokens // 4)

        x0s = perm(x0, swap)
        x1s = perm(x1, swap)
        x3 = perm(x1, near)
        x3s = perm(x3, swap)

        dirn = jnp.where(core == 0, 1, -1)

        def src(off, k):
            return 2 * ((chip + off + chips) % chips) + k

        def one_pass(xa, xb, off_a, off_b, b_dtype=jnp.float32):
            ids = jnp.stack([src(off_a, core), src(off_b, 1 - core)]).astype(jnp.int32)
            sums = expert_pass(ids, xa, xb, tok_all, gate_all, w_gate, w_up, w_down, cap, b_dtype)
            return [v.reshape(xa.shape) for v in sums]

        def add(pa, q, dep):
            return add_partials(after(pa, dep), q)

        y = shared_piece(None, tok, 0, 2)
        pa1, pb1 = one_pass(after(x1, y, x1s), x1s, dirn, -dirn)
        x2 = perm(after(x0, pa1), far)
        x2s = perm(x2, swap)
        q1 = perm(pb1, swap)
        pa2, pb2 = one_pass(after(x3, pa1), x3s, 2, 2)
        q2 = perm(pb2, swap)
        c1 = add(pa1, q1, pa2)
        r1 = perm(c1, far)
        c2 = add(pa2, q2, c1)
        r2 = perm(c2, across)
        pa3, pb3 = one_pass(after(x2, c2), x2s, -dirn, dirn)
        q3 = perm(pb3, swap)
        y = shared_piece(y, pa3, 2, 3)
        c3 = add(pa3, q3, y)
        r3 = perm(c3, near)
        pa4, pb4 = one_pass(after(x0, c3), x0s, 0, 0, jnp.bfloat16)
        q4 = perm(pb4, swap)
        y = shared_piece(y, (pa4, pb4), 3, 4)
        return finish(y, pa4, q4, r1, r2, r3)

    return jax.shard_map(device_fn, mesh=mesh, in_specs=(tok_spec, P(), bank_spec, bank_spec, bank_spec, P(), P(), P(), tok_spec, tok_spec), out_specs=tok_spec, check_vma=False)
```
